256 devices in a mesh: dp: 32 (over z, y), chan: 8 (over x, core).
Axes of the slice: x: 4, y: 4, z: 8, core: 2. Of those that a mesh axis runs over, the one named last changes fastest.
Arguments:
- activations: bfloat16 [32, 16, 64, 1024], P('dp', None, None, 'chan'), may hold values from -60 to 60
- cotangent: bfloat16 [32, 16, 64, 1024], P('dp', None, None, 'chan'), may hold values from -6 to 6
- dw_kernel: float32 [49, 1024], P(None, 'chan'), may hold values from -0.875 to 0.875
- norm_gain: float32 [4, 1024], P(None, 'chan'), may hold values from 0.1 to 1.9
- norm_bias: float32 [4, 1024], P(None, 'chan'), may hold values from -3 to 3
- w_in: bfloat16 [1024, 4096], P(None, 'chan'), may hold values from -0.1875 to 0.1875
- b_in: float32 [4096], P('chan'), may hold values from -3 to 3
- w_out: bfloat16 [4096, 1024], P('chan'), may hold values from -0.09375 to 0.09375
- layer_scale: float32 [1024], P('chan'), may hold values from 0.3 to 1.5
- group_sizes: int32 [4], replicated, may hold values from 1 to 16, 32 in all
Outputs:
- result: bfloat16 [32, 16, 64, 1024], P('dp', None, None, 'chan')
- d_input: bfloat16 [32, 16, 64, 1024], P('dp', None, None, 'chan')
- d_kernel: float32 [49, 1024], P(None, 'chan')
- d_gain: float32 [4, 1024], P(None, 'chan')
- d_bias: float32 [4, 1024], P(None, 'chan')
- d_w_in: float32 [1024, 4096], P('dp', 'chan')
- d_b_in: float32 [4096], P('chan')
- d_w_out: float32 [4096, 1024], P('chan', 'dp')
- d_scale: float32 [1024], P('chan')
The draws below stay inside these ranges and needn't reach their ends.
Inputs may be any that keep to these rules, and one draw needn't show every extreme that they name: `group_sizes`: the sizes sum to 32, each is at least one, and the largest is exactly 16.
All inputs are finite; a program needn't handle non-finite values.
Results may differ from the reference program's by a relative error of at most 0.015.
Values may be sent and summed in bfloat16 or wider, within the bound.
No kernel may reach another device: no remote copies, remote signals or barrier semaphores. Data moves between devices by JAX's collectives and lax.ppermute only.
A program may use at most 128 MiB of HBM per device.

```python
import math
import jax
import jax.numpy as jnp
import numpy as np
from jax import lax

C = 1024
HID = 4096
KS = 7
IMG_H = 16
IMG_W = 64
GROUPS = 4
IMAGES = 32
N_DP = 32
N_CHAN = 8


def draw_activations(key, part):
    subkeys = jax.random.split(jax.random.fold_in(key, 17), 4)
    full_shape = (IMAGES, IMG_H, IMG_W, C)
    rising = 3.0 ** (jnp.arange(IMAGES, dtype=jnp.float32) / (IMAGES - 1))
    texture = jnp.exp(jax.random.uniform(subkeys[3], (1, IMG_H, IMG_W, 1), jnp.float32, -0.35, 0.35))
    values = jnp.clip(jax.random.normal(subkeys[0], full_shape, jnp.float32), -4.0, 4.0)
    spread = 0.3 * jnp.exp(jax.random.uniform(subkeys[1], (C,), jnp.float32, 0.0, math.log(10.0)))
    mixed = values * texture * spread * rising[:, None, None, None]
    return mixed.astype(jnp.bfloat16)


def level_of(rng, dims, cuts, low, top_value):
    level = 1.0
    for position, blocks in cuts:
        draws = jax.random.uniform(jax.random.fold_in(jax.random.fold_in(rng, 6), position), (blocks,), jnp.float32, low / len(cuts), top_value / len(cuts))
        level = level * jnp.repeat(jnp.exp(draws), dims[position] // blocks).reshape((-1,) + (1,) * (len(dims) - 1 - position))
    return level


def profile(amount, total, bound, lean):
    portions = [(1 << 20) // math.isqrt(standing ** lean) + 1 for standing in range(2, amount + 1)]
    spare, given = total - bound - (amount - 1), [1] * (amount - 1)
    while spare > 0:
        candidates = [i for i in range(amount - 1) if given[i] < bound]
        whole, budget = sum([portions[i] for i in candidates]), spare
        for i in candidates:
            more = min(bound - given[i], max(1, budget * portions[i] // whole), spare)
            given[i] = given[i] + more
            spare = spare - more
    return np.array([bound] + given)


def ragged_sizes(rng, number_of, total, limit, skew):
    if number_of == 2:
        one = jax.random.randint(rng, (), max(1, total - limit), min(limit, total - 1) + 1)
        return jnp.stack([one, total - one])
    tallies = jnp.asarray(profile(number_of, total, limit, skew), jnp.int32)
    twos = (number_of - 1) // 2
    source_of, taker = tallies[1:1 + 2 * twos:2], tallies[2:2 + 2 * twos:2]
    margin = jnp.minimum(source_of - 1, limit - taker)
    passed = jax.random.randint(jax.random.fold_in(rng, 1), (twos,), 0, 1 << 20) % (margin + 1)
    tallies = tallies.at[1:1 + 2 * twos:2].set(source_of - passed).at[2:2 + 2 * twos:2].set(taker + passed)
    return tallies[jax.random.permutation(jax.random.fold_in(rng, 2), number_of)]


def bell_draw(key, shape, scale, most, cuts=(), kind=jnp.bfloat16):
    drawn = scale * jax.random.normal(key, shape, jnp.float32)
    if cuts:
        drawn = drawn * level_of(key, shape, cuts, -0.22, 0.18)
    return jnp.clip(drawn, -most, most).astype(kind)


def setup_inputs(seed: int = 0) -> dict:
    arg_keys = jax.random.split(jax.random.key(seed), 11)
    activations = draw_activations(jax.random.fold_in(arg_keys[10], 71), 0)
    cotangent = bell_draw(arg_keys[1], (IMAGES, IMG_H, IMG_W, C), 1.0, 6.0, ((0, 32), (3, 8)))
    dw_kernel = bell_draw(arg_keys[2], (KS * KS, C), (KS * KS) ** -0.5, 0.875, ((1, 8),), jnp.float32)
    norm_gain = jnp.clip(1.0 + 0.18 * jax.random.normal(arg_keys[3], (GROUPS, C), jnp.float32), 0.1, 1.9)
    norm_bias = bell_draw(arg_keys[4], (GROUPS, C), 0.5, 3.0, ((1, 8),), jnp.float32)
    w_in = bell_draw(arg_keys[5], (C, HID), C ** -0.5, 0.1875, ((1, 8),))
    b_in = bell_draw(arg_keys[6], (HID,), 0.5, 3.0, ((0, 8),), jnp.float32)
    w_out = bell_draw(arg_keys[7], (HID, C), HID ** -0.5, 0.09375, ((0, 8),))
    layer_scale = jnp.clip(jnp.exp(math.log(1.5) - 1.60943787 * jax.random.uniform(arg_keys[8], (C,), jnp.float32) ** level_of(arg_keys[8], (C,), ((0, 8),), -0.2, 0.2)), 0.3, 1.5)
    group_sizes = ragged_sizes(arg_keys[9], GROUPS, N_DP, N_DP // 2, 2).astype(jnp.int32)
    return dict(activations=activations, cotangent=cotangent, dw_kernel=dw_kernel, norm_gain=norm_gain, norm_bias=norm_bias, w_in=w_in, b_in=b_in, w_out=w_out, layer_scale=layer_scale, group_sizes=group_sizes)


EPS = 1e-05

def depthwise(field, kernel):
    reach = KS // 2
    height, width = (field.shape[1], field.shape[2])
    padded = jnp.pad(field, ((0, 0), (reach, reach), (reach, reach), (0, 0)))
    running = jnp.zeros(field.shape, jnp.float32)
    for shift_row in range(KS):
        for shift_col in range(KS):
            window = padded[:, shift_row:shift_row + height, shift_col:shift_col + width, :]
            running = running + window * kernel[shift_row * KS + shift_col]
    return running

def kernel_grad(field, upstream):
    reach = KS // 2
    height, width = (field.shape[1], field.shape[2])
    padded = jnp.pad(field, ((0, 0), (reach, reach), (reach, reach), (0, 0)))
    collected = []
    for shift_row in range(KS):
        for shift_col in range(KS):
            window = padded[:, shift_row:shift_row + height, shift_col:shift_col + width, :]
            collected.append(lax.optimization_barrier(jnp.sum(window * upstream, axis=(0, 1, 2))))
    return jnp.stack(collected)

def group_member(group_sizes, number):
    group_ends = jnp.cumsum(group_sizes)
    positions = jnp.arange(number, dtype=jnp.int32)
    labels = lax.optimization_barrier(jnp.sum((group_ends[None, :] <= positions[:, None]).astype(jnp.int32), axis=1))
    return (labels[:, None] == jnp.arange(group_sizes.shape[0], dtype=jnp.int32)[None, :]).astype(jnp.float32)

def select(member, table):
    return lax.optimization_barrier(jnp.sum(member[:, :, None] * table[None], axis=1))

def reference(activations, cotangent, dw_kernel, norm_gain, norm_bias, w_in, b_in, w_out, layer_scale, group_sizes):
    images = activations.shape[0]
    row_count = IMG_H * IMG_W
    member = group_member(group_sizes, images)
    counts = group_sizes.astype(jnp.float32) * row_count
    source = activations.astype(jnp.float32)
    filtered = depthwise(source, dw_kernel).reshape(images, row_count, C)
    firsts = lax.optimization_barrier(jnp.sum(filtered, axis=1))
    seconds = lax.optimization_barrier(jnp.sum(filtered * filtered, axis=1))
    group_mean = lax.optimization_barrier(jnp.sum(member[:, :, None] * firsts[:, None, :], axis=0)) / counts[:, None]
    group_var = lax.optimization_barrier(jnp.sum(member[:, :, None] * seconds[:, None, :], axis=0)) / counts[:, None] - group_mean * group_mean
    group_rstd = lax.rsqrt(group_var + EPS)
    image_mean = select(member, group_mean)
    image_rstd = select(member, group_rstd)
    image_gain = select(member, norm_gain)
    image_bias = select(member, norm_bias)
    image_count = lax.optimization_barrier(jnp.sum(member * counts[None, :], axis=1))
    centered = (filtered - image_mean[:, None, :]) * image_rstd[:, None, :]
    normed = (centered * image_gain[:, None, :] + image_bias[:, None, :]).astype(jnp.bfloat16)
    upstream = cotangent.reshape(images, row_count, C)
    plain = source.reshape(images, row_count, C)
    block = HID // N_CHAN
    in_blocks = w_in.astype(jnp.float32).reshape(C, N_CHAN, block).transpose(1, 0, 2)
    out_blocks = w_out.astype(jnp.float32).reshape(N_CHAN, block, C)
    contract_rows = (((0,), (0,)), ((), ()))
    contract_cols = (((1,), (1,)), ((), ()))

    def step(carry, inputs):
        grad_in, grad_out, grad_bias, grad_scale = carry
        features, incoming, initial = inputs
        hidden = jnp.dot(features, w_in, preferred_element_type=jnp.float32) + b_in
        activated = jax.nn.gelu(hidden).astype(jnp.bfloat16)
        pieces = jnp.einsum('rnh,nhc->nrc', activated.astype(jnp.float32).reshape(row_count, N_CHAN, block), out_blocks, precision=lax.Precision.HIGHEST)
        rounded = lax.optimization_barrier(pieces.astype(jnp.bfloat16))
        branch = lax.optimization_barrier(jnp.sum(rounded.astype(jnp.float32), axis=0))
        incoming_f = incoming.astype(jnp.float32)
        output_rows = (initial + layer_scale * branch).astype(jnp.bfloat16)
        grad_scale = grad_scale + lax.optimization_barrier(jnp.sum(incoming_f * branch, axis=0))
        d_branch = (incoming_f * layer_scale).astype(jnp.bfloat16)
        grad_out = grad_out + lax.dot_general(activated, d_branch, contract_rows, preferred_element_type=jnp.float32)
        d_activated = lax.dot_general(d_branch, w_out, contract_cols, preferred_element_type=jnp.float32)
        _, pullback = jax.vjp(jax.nn.gelu, hidden)
        d_hidden = pullback(d_activated)[0]
        grad_bias = grad_bias + lax.optimization_barrier(jnp.sum(d_hidden, axis=0))
        hidden_b = d_hidden.astype(jnp.bfloat16)
        grad_in = grad_in + lax.dot_general(features, hidden_b, contract_rows, preferred_element_type=jnp.float32)
        backward = jnp.einsum('rnh,nch->nrc', hidden_b.astype(jnp.float32).reshape(row_count, N_CHAN, block), in_blocks, precision=lax.Precision.HIGHEST)
        d_normed = lax.optimization_barrier(jnp.sum(lax.optimization_barrier(backward.astype(jnp.bfloat16)).astype(jnp.float32), axis=0))
        return ((grad_in, grad_out, grad_bias, grad_scale), (output_rows, d_normed))
    start = (jnp.zeros((C, HID), jnp.float32), jnp.zeros((HID, C), jnp.float32), jnp.zeros((HID,), jnp.float32), jnp.zeros((C,), jnp.float32))
    finals, outputs = lax.scan(step, start, (normed, upstream, plain))
    grad_in, grad_out, grad_bias, grad_scale = finals
    output_rows, d_normed = outputs
    gain_terms = lax.optimization_barrier(jnp.sum(d_normed * centered, axis=1))
    bias_terms = lax.optimization_barrier(jnp.sum(d_normed, axis=1))
    d_gain = lax.optimization_barrier(jnp.sum(member[:, :, None] * gain_terms[:, None, :], axis=0))
    d_bias = lax.optimization_barrier(jnp.sum(member[:, :, None] * bias_terms[:, None, :], axis=0))
    image_dgain = select(member, d_gain)
    image_dbias = select(member, d_bias)
    scaled = image_gain[:, None, :] * image_rstd[:, None, :]
    d_filtered = scaled * (d_normed - image_dbias[:, None, :] / image_count[:, None, None] - centered * image_dgain[:, None, :] / image_count[:, None, None])
    d_filtered = d_filtered.reshape(images, IMG_H, IMG_W, C)
    d_kernel = kernel_grad(source, d_filtered)
    d_input = (cotangent.astype(jnp.float32) + depthwise(d_filtered, dw_kernel[::-1])).astype(jnp.bfloat16)
    result = output_rows.reshape(images, IMG_H, IMG_W, C)
    return (result, d_input, d_kernel, d_gain, d_bias, grad_in, grad_bias, grad_out, grad_scale)
```

```python
import jax
import jax.numpy as jnp
from jax import lax
from jax.sharding import Mesh
from jax.sharding import PartitionSpec as P

KS = 7
DP = ("z", "y")
CH = ("x", "c")
SWAP = [(0, 1), (1, 0)]
EPS = 1e-05


def sent_to_all(array, axis):
    size = lax.axis_size(axis)
    return lax.all_to_all(
        jnp.broadcast_to(array[None], (size, *array.shape)), axis, 0, 0, tiled=True
    )


def packed_total(arrays, axis):
    ends = [0]
    for a in arrays:
        ends.append(ends[-1] + a.size)
    everything = sent_to_all(jnp.concatenate([a.ravel() for a in arrays]), axis)
    total = jnp.sum(everything, axis=0)
    return tuple((total[b:e].reshape(a.shape) for a, b, e in zip(arrays, ends, ends[1:])))


def depthwise(field, kernel):
    reach = KS // 2
    height, width = (field.shape[1], field.shape[2])
    padded = jnp.pad(field, ((0, 0), (reach, reach), (reach, reach), (0, 0)))
    running = jnp.zeros(field.shape, jnp.float32)
    for shift_row in range(KS):
        for shift_col in range(KS):
            window = padded[:, shift_row : shift_row + height, shift_col : shift_col + width, :]
            running = running + window * kernel[shift_row * KS + shift_col]
    return running


def kernel_grad(field, upstream):
    reach = KS // 2
    height, width = (field.shape[1], field.shape[2])
    padded = jnp.pad(field, ((0, 0), (reach, reach), (reach, reach), (0, 0)))
    collected = []
    for shift_row in range(KS):
        for shift_col in range(KS):
            window = padded[:, shift_row : shift_row + height, shift_col : shift_col + width, :]
            collected.append(jnp.sum(window * upstream, axis=(0, 1, 2)))
    return jnp.stack(collected)


def rows_of_all(array):
    rows, own = array.shape
    halves = jnp.broadcast_to(array.reshape(1, 2, rows // 2, own), (4, 2, rows // 2, own))
    pieces = lax.all_to_all(halves.reshape(8, rows // 2, own), CH, 0, 0, tiled=True)
    return jnp.moveaxis(pieces, 0, 1).reshape(rows // 2, 8 * own)


def summed_to_owner(array):
    rows, width = array.shape
    own = width // 8
    pieces = jnp.moveaxis(array.reshape(rows, 8, own), 1, 0)
    pieces = lax.all_to_all(pieces, CH, 0, 0, tiled=True).reshape(4, 2 * rows, own)
    return jnp.sum(pieces.astype(jnp.float32), axis=0)


def body(
    activations,
    cotangent,
    dw_kernel,
    norm_gain,
    norm_bias,
    w_in,
    b_in,
    w_out,
    layer_scale,
    group_sizes,
):
    height, width, channels = (activations.shape[1], activations.shape[2], activations.shape[3])
    row_count = height * width
    half = row_count // 2
    core = lax.axis_index("c")
    devices = lax.axis_size(DP)
    position = lax.axis_index(DP)
    groups = group_sizes.shape[0]
    group_ends = jnp.cumsum(group_sizes)
    positions = jnp.arange(devices, dtype=jnp.int32)
    labels = jnp.sum((group_ends[None, :] <= positions[:, None]).astype(jnp.int32), axis=1)
    own_group = jnp.sum((group_ends <= position).astype(jnp.int32))
    owners = (jnp.arange(groups, dtype=jnp.int32)[:, None] == labels[None, :]).astype(jnp.float32)
    mates = (labels == own_group).astype(jnp.float32)
    member = (jnp.arange(groups, dtype=jnp.int32) == own_group).astype(jnp.float32)
    own_count = jnp.sum(member * group_sizes.astype(jnp.float32)) * row_count
    own_gain = jnp.sum(member[:, None] * norm_gain, axis=0)
    own_bias = jnp.sum(member[:, None] * norm_bias, axis=0)

    incoming = cotangent.reshape(row_count, channels).astype(jnp.float32)
    d_branch = (incoming * layer_scale).astype(jnp.bfloat16)
    everyone = lax.all_gather(d_branch, CH, axis=0, tiled=False)
    mine = lax.dynamic_slice_in_dim(everyone, core * half, half, axis=1)
    branch_full = jnp.moveaxis(mine, 0, 1).reshape(half, 8 * channels)
    w_in_pair = lax.ppermute(w_in, "c", SWAP)
    w_out_pair = lax.ppermute(w_out, "c", SWAP)
    b_in_pair = lax.ppermute(b_in, "c", SWAP)

    source = activations.astype(jnp.float32)
    filtered = depthwise(source, dw_kernel).reshape(row_count, channels)
    moments = jnp.stack([jnp.sum(filtered, axis=0), jnp.sum(filtered * filtered, axis=0)])
    per_device = sent_to_all(moments, DP)
    totals = jnp.sum(mates[:, None, None] * per_device, axis=0)
    own_mean = totals[0] / own_count
    own_var = totals[1] / own_count - own_mean * own_mean
    own_rstd = lax.rsqrt(own_var + EPS)
    centered = (filtered - own_mean) * own_rstd
    normed = (centered * own_gain + own_bias).astype(jnp.bfloat16)
    gathered = rows_of_all(normed)

    contract_rows = (((0,), (0,)), ((), ()))
    contract_cols = (((1,), (1,)), ((), ()))

    def dot(a, b, dims):
        return lax.dot_general(a, b, dims, preferred_element_type=jnp.float32)

    def forward(weights, bias):
        hidden = jnp.dot(gathered, weights, preferred_element_type=jnp.float32) + bias
        return hidden, jax.nn.gelu(hidden).astype(jnp.bfloat16)

    hidden_own, active_own = forward(w_in, b_in)
    hidden_pair, active_pair = forward(w_in_pair, b_in_pair)

    def upstream(hidden, weights):
        _, pullback = jax.vjp(jax.nn.gelu, hidden)
        grad = pullback(dot(branch_full, weights, contract_cols))[0]
        return jnp.sum(grad, axis=0), grad.astype(jnp.bfloat16)

    bias_own, back_own = upstream(hidden_own, w_out)
    bias_pair, back_pair = upstream(hidden_pair, w_out_pair)
    partial_normed = dot(back_own, w_in, contract_cols) + dot(back_pair, w_in_pair, contract_cols)
    d_normed = summed_to_owner(partial_normed.astype(jnp.bfloat16))

    def weight_grads(active, back):
        out_t = dot(branch_full, active, contract_rows)
        inner = dot(gathered, back, contract_rows)
        return jnp.concatenate([inner, out_t], axis=1)

    for_pair = weight_grads(active_pair, back_pair).astype(jnp.bfloat16)
    from_pair = lax.ppermute(for_pair, "c", SWAP)
    both_local = weight_grads(active_own, back_own) + from_pair.astype(jnp.float32)
    both_sums = lax.psum_scatter(
        both_local.astype(jnp.bfloat16), "z", scatter_dimension=0, tiled=True
    )
    both_sums = lax.psum_scatter(both_sums, "y", scatter_dimension=0, tiled=True)
    both_sums = both_sums.astype(jnp.float32)
    hidden_cols = w_in.shape[1]
    d_w_in = both_sums[:, :hidden_cols]
    d_w_out = both_sums[:, hidden_cols:].T
    bias_local = bias_own + lax.ppermute(bias_pair, "c", SWAP)

    partial_branch = jnp.dot(active_own, w_out, preferred_element_type=jnp.float32) + jnp.dot(
        active_pair, w_out_pair, preferred_element_type=jnp.float32
    )
    branch = summed_to_owner(partial_branch.astype(jnp.bfloat16))
    initial = source.reshape(row_count, channels)
    result = (initial + layer_scale * branch).astype(jnp.bfloat16).reshape(activations.shape)
    scale_local = jnp.sum(incoming * branch, axis=0)

    grad_moments = jnp.stack([jnp.sum(d_normed * centered, axis=0), jnp.sum(d_normed, axis=0)])
    grad_rows = sent_to_all(grad_moments, DP)
    grad_totals = jnp.sum(owners[:, :, None, None] * grad_rows[None], axis=1)
    d_gain = grad_totals[:, 0]
    d_bias = grad_totals[:, 1]
    own_dgain = jnp.sum(member[:, None] * d_gain, axis=0)
    own_dbias = jnp.sum(member[:, None] * d_bias, axis=0)
    d_filtered = (
        own_gain * own_rstd * (d_normed - own_dbias / own_count - centered * own_dgain / own_count)
    )
    d_filtered = d_filtered.reshape(activations.shape)
    kernel_local = kernel_grad(source, d_filtered)
    d_kernel, d_b_in, d_scale = packed_total((kernel_local, bias_local, scale_local), DP)
    d_input = (cotangent.astype(jnp.float32) + depthwise(d_filtered, dw_kernel[::-1])).astype(
        jnp.bfloat16
    )
    return (result, d_input, d_kernel, d_gain, d_bias, d_w_in, d_b_in, d_w_out, d_scale)


def solution(mesh):
    split = Mesh(mesh.devices.reshape(8, 4, 4, 2), ("z", "y", "x", "c"))
    in_specs = (
        P(DP, None, None, CH),
        P(DP, None, None, CH),
        P(None, CH),
        P(None, CH),
        P(None, CH),
        P(None, CH),
        P(CH),
        P(CH, None),
        P(CH),
        P(),
    )
    out_specs = (
        P(DP, None, None, CH),
        P(DP, None, None, CH),
        P(None, CH),
        P(None, CH),
        P(None, CH),
        P(DP, CH),
        P(CH),
        P(CH, DP),
        P(CH),
    )
    return jax.shard_map(body, mesh=split, in_specs=in_specs, out_specs=out_specs, check_vma=False)
```

```python
import jax
import jax.numpy as jnp
from jax import lax
from jax.sharding import Mesh
from jax.sharding import PartitionSpec as P

KS = 7
DP = ("z", "y")
CH = ("x", "c")
SWAP = [(0, 1), (1, 0)]
EPS = 1e-05


def sent_to_all(array, axis):
    size = lax.axis_size(axis)
    return lax.all_to_all(
        jnp.broadcast_to(array[None], (size, *array.shape)), axis, 0, 0, tiled=True
    )


def packed_total(arrays, axis):
    ends = [0]
    for a in arrays:
        ends.append(ends[-1] + a.size)
    everything = sent_to_all(jnp.concatenate([a.ravel() for a in arrays]), axis)
    total = jnp.sum(everything, axis=0)
    return tuple((total[b:e].reshape(a.shape) for a, b, e in zip(arrays, ends, ends[1:])))


def depthwise(field, kernel):
    reach = KS // 2
    height, width = (field.shape[1], field.shape[2])
    padded = jnp.pad(field, ((0, 0), (reach, reach), (reach, reach), (0, 0)))
    running = jnp.zeros(field.shape, jnp.float32)
    for shift_row in range(KS):
        for shift_col in range(KS):
            window = padded[:, shift_row : shift_row + height, shift_col : shift_col + width, :]
            running = running + window * kernel[shift_row * KS + shift_col]
    return running


def kernel_grad(field, upstream):
    reach = KS // 2
    height, width = (field.shape[1], field.shape[2])
    padded = jnp.pad(field, ((0, 0), (reach, reach), (reach, reach), (0, 0)))
    collected = []
    for shift_row in range(KS):
        for shift_col in range(KS):
            window = padded[:, shift_row : shift_row + height, shift_col : shift_col + width, :]
            collected.append(jnp.sum(window * upstream, axis=(0, 1, 2)))
    return jnp.stack(collected)


def rows_of_all(array):
    rows, own = array.shape
    halves = jnp.broadcast_to(array.reshape(1, 2, rows // 2, own), (4, 2, rows // 2, own))
    pieces = lax.all_to_all(halves.reshape(8, rows // 2, own), CH, 0, 0, tiled=True)
    return jnp.moveaxis(pieces, 0, 1).reshape(rows // 2, 8 * own)


def exchanged(array):
    rows, width = array.shape
    own = width // 8
    pieces = jnp.moveaxis(array.reshape(rows, 8, own), 1, 0)
    return lax.all_to_all(pieces, CH, 0, 0, tiled=True).reshape(4, 2 * rows, own)


def summed(pieces):
    return jnp.sum(pieces.astype(jnp.float32), axis=0)


def body(
    activations,
    cotangent,
    dw_kernel,
    norm_gain,
    norm_bias,
    w_in,
    b_in,
    w_out,
    layer_scale,
    group_sizes,
):
    height, width, channels = (activations.shape[1], activations.shape[2], activations.shape[3])
    row_count = height * width
    half = row_count // 2
    core = lax.axis_index("c")
    devices = lax.axis_size(DP)
    position = lax.axis_index(DP)
    groups = group_sizes.shape[0]
    group_ends = jnp.cumsum(group_sizes)
    positions = jnp.arange(devices, dtype=jnp.int32)
    labels = jnp.sum((group_ends[None, :] <= positions[:, None]).astype(jnp.int32), axis=1)
    own_group = jnp.sum((group_ends <= position).astype(jnp.int32))
    owners = (jnp.arange(groups, dtype=jnp.int32)[:, None] == labels[None, :]).astype(jnp.float32)
    mates = (labels == own_group).astype(jnp.float32)
    member = (jnp.arange(groups, dtype=jnp.int32) == own_group).astype(jnp.float32)
    own_count = jnp.sum(member * group_sizes.astype(jnp.float32)) * row_count
    own_gain = jnp.sum(member[:, None] * norm_gain, axis=0)
    own_bias = jnp.sum(member[:, None] * norm_bias, axis=0)

    incoming = cotangent.reshape(row_count, channels).astype(jnp.float32)
    d_branch = (incoming * layer_scale).astype(jnp.bfloat16)
    everyone = lax.all_gather(d_branch, CH, axis=0, tiled=False)
    mine = lax.dynamic_slice_in_dim(everyone, core * half, half, axis=1)
    branch_full = jnp.moveaxis(mine, 0, 1).reshape(half, 8 * channels)
    w_in_pair = lax.ppermute(w_in, "c", SWAP)
    w_out_pair = lax.ppermute(w_out, "c", SWAP)
    b_in_pair = lax.ppermute(b_in, "c", SWAP)

    source = activations.astype(jnp.float32)
    filtered = depthwise(source, dw_kernel).reshape(row_count, channels)
    moments = jnp.stack([jnp.sum(filtered, axis=0), jnp.sum(filtered * filtered, axis=0)])
    per_device = sent_to_all(moments, DP)
    totals = jnp.sum(mates[:, None, None] * per_device, axis=0)
    own_mean = totals[0] / own_count
    own_var = totals[1] / own_count - own_mean * own_mean
    own_rstd = lax.rsqrt(own_var + EPS)
    centered = (filtered - own_mean) * own_rstd
    normed = (centered * own_gain + own_bias).astype(jnp.bfloat16)
    gathered = rows_of_all(normed)

    contract_rows = (((0,), (0,)), ((), ()))
    contract_cols = (((1,), (1,)), ((), ()))

    def dot(a, b, dims):
        return lax.dot_general(a, b, dims, preferred_element_type=jnp.float32)

    def forward(weights, bias):
        hidden = jnp.dot(gathered, weights, preferred_element_type=jnp.float32) + bias
        return hidden, jax.nn.gelu(hidden).astype(jnp.bfloat16)

    hidden_own, active_own = forward(w_in, b_in)
    hidden_pair, active_pair = forward(w_in_pair, b_in_pair)

    partial_branch = jnp.dot(active_own, w_out, preferred_element_type=jnp.float32) + jnp.dot(
        active_pair, w_out_pair, preferred_element_type=jnp.float32
    )
    branch_pieces = exchanged(partial_branch.astype(jnp.bfloat16))
    branch = summed(branch_pieces)
    initial = source.reshape(row_count, channels)
    result = (initial + layer_scale * branch).astype(jnp.bfloat16).reshape(activations.shape)
    scale_local = jnp.sum(incoming * branch, axis=0)

    def upstream(hidden, weights):
        _, pullback = jax.vjp(jax.nn.gelu, hidden)
        grad = pullback(dot(branch_full, weights, contract_cols))[0]
        return jnp.sum(grad, axis=0), grad.astype(jnp.bfloat16)

    bias_own, back_own = upstream(hidden_own, w_out)
    bias_pair, back_pair = upstream(hidden_pair, w_out_pair)
    partial_normed = dot(back_own, w_in, contract_cols) + dot(back_pair, w_in_pair, contract_cols)
    partial_normed, branch_pieces = lax.optimization_barrier(
        (partial_normed.astype(jnp.bfloat16), branch_pieces)
    )
    normed_pieces = exchanged(partial_normed)

    def weight_grads(active, back):
        out_t = dot(branch_full, active, contract_rows)
        inner = dot(gathered, back, contract_rows)
        return jnp.concatenate([inner, out_t], axis=1)

    for_pair = weight_grads(active_pair, back_pair).astype(jnp.bfloat16)
    from_pair = lax.ppermute(for_pair, "c", SWAP)
    both_local = weight_grads(active_own, back_own) + from_pair.astype(jnp.float32)
    both_local = both_local.astype(jnp.bfloat16)
    near = lax.psum_scatter(both_local, "z", scatter_dimension=0, tiled=True)
    hidden_cols = w_in.shape[1]
    bias_local = bias_own + lax.ppermute(bias_pair, "c", SWAP)
    normed_pieces, both_local = lax.optimization_barrier((normed_pieces, both_local))
    d_normed = summed(normed_pieces)

    grad_moments = jnp.stack([jnp.sum(d_normed * centered, axis=0), jnp.sum(d_normed, axis=0)])
    grad_rows = sent_to_all(grad_moments, DP)
    grad_totals = jnp.sum(owners[:, :, None, None] * grad_rows[None], axis=1)
    d_gain = grad_totals[:, 0]
    d_bias = grad_totals[:, 1]
    own_dgain = jnp.sum(member[:, None] * d_gain, axis=0)
    own_dbias = jnp.sum(member[:, None] * d_bias, axis=0)
    d_filtered = (
        own_gain * own_rstd * (d_normed - own_dbias / own_count - centered * own_dgain / own_count)
    )
    d_filtered = d_filtered.reshape(activations.shape)
    kernel_local = kernel_grad(source, d_filtered)
    d_kernel, d_b_in, d_scale = packed_total((kernel_local, bias_local, scale_local), DP)
    near, d_kernel = lax.optimization_barrier((near, d_kernel))
    everything = lax.all_to_all(near.reshape(4, -1, near.shape[1]), "y", 0, 0, tiled=True)
    both_sums = jnp.sum(everything.astype(jnp.float32), axis=0)
    d_w_in = both_sums[:, :hidden_cols]
    d_w_out = both_sums[:, hidden_cols:].T
    d_input = (cotangent.astype(jnp.float32) + depthwise(d_filtered, dw_kernel[::-1])).astype(
        jnp.bfloat16
    )
    return (result, d_input, d_kernel, d_gain, d_bias, d_w_in, d_b_in, d_w_out, d_scale)


def solution(mesh):
    split = Mesh(mesh.devices.reshape(8, 4, 4, 2), ("z", "y", "x", "c"))
    in_specs = (
        P(DP, None, None, CH),
        P(DP, None, None, CH),
        P(None, CH),
        P(None, CH),
        P(None, CH),
        P(None, CH),
        P(CH),
        P(CH, None),
        P(CH),
        P(),
    )
    out_specs = (
        P(DP, None, None, CH),
        P(DP, None, None, CH),
        P(None, CH),
        P(None, CH),
        P(None, CH),
        P(DP, CH),
        P(CH),
        P(CH, DP),
        P(CH),
    )
    return jax.shard_map(body, mesh=split, in_specs=in_specs, out_specs=out_specs, check_vma=False)
```

```python
import jax
import jax.numpy as jnp
from jax import lax
from jax.experimental import pallas as pl
from jax.experimental.pallas import tpu as pltpu
from jax.sharding import Mesh
from jax.sharding import PartitionSpec as P


KS = 7
DP = ("z", "y")
CH = ("x", "c")
SWAP = [(0, 1), (1, 0)]
EPS = 1e-05


def sent_to_all(array, axis):
    size = lax.axis_size(axis)
    return lax.all_to_all(
        jnp.broadcast_to(array[None], (size, *array.shape)), axis, 0, 0, tiled=True
    )


def rows_of_all(array):
    rows, own = array.shape
    halves = jnp.broadcast_to(array.reshape(1, 2, rows // 2, own), (4, 2, rows // 2, own))
    return lax.all_to_all(halves.reshape(8, rows // 2, own), CH, 0, 0, tiled=True)


def exchanged(pieces):
    _, rows, own = pieces.shape
    return lax.all_to_all(pieces, CH, 0, 0, tiled=True).reshape(4, 2 * rows, own)


def summed(pieces):
    return jnp.sum(pieces.astype(jnp.float32), axis=0)


REACH = KS // 2
TAPS = KS * KS


def spread(field, pad, planes):
    height, width, lanes = field.shape
    pad[:, :8] = jnp.zeros((height, 8, lanes), jnp.float32)
    pad[:, width + 8 :] = jnp.zeros((height, 8, lanes), jnp.float32)
    edge = jnp.zeros((KS, REACH, width, lanes), jnp.float32)
    planes[:, :REACH] = edge
    planes[:, height + REACH :] = edge

    @pl.loop(0, height)
    def _(r):
        pad[r, 8 : width + 8] = field[r].astype(jnp.float32)
        for b in range(KS):
            planes[b, r + REACH] = pad[r, 8 - REACH + b : 8 - REACH + b + width]


def filtered_row(planes, kernel, r, reverse=False):
    total = None
    for a in range(KS):
        for b in range(KS):
            tap = a * KS + b
            tap = TAPS - 1 - tap if reverse else tap
            term = planes[b, r + a] * kernel[tap : tap + 1]
            total = term if total is None else total + term
    return total


def folded(value):
    return jnp.sum(value.reshape(-1, 8, value.shape[-1]), axis=0)


def tap_sums(planes, upstream, height, out, plain=None):
    out[...] = jnp.zeros_like(out)
    if plain is not None:
        plain[...] = jnp.zeros_like(plain)
    zero = jnp.zeros((8, out.shape[1]), jnp.float32)
    for b in range(KS):

        def step(r, sums):
            u = upstream(r)
            sums = list(sums)
            for a in range(KS):
                window = planes[b, r + a]
                sums[a] = sums[a] + folded(window * u)
                if plain is not None:
                    sums[KS + a] = sums[KS + a] + folded(window)
            return tuple(sums)

        sums = lax.fori_loop(0, height, step, (zero,) * (KS if plain is None else 2 * KS))
        for a in range(KS):
            tap = a * KS + b
            out[tap : tap + 1] = jnp.sum(sums[a], axis=0, keepdims=True)
            if plain is not None:
                plain[tap : tap + 1] = jnp.sum(sums[KS + a], axis=0, keepdims=True)


def filter_kernel(source, kernel, filtered, moments, pad, planes):
    spread(source, pad, planes)
    zero = jnp.zeros((8, kernel.shape[1]), jnp.float32)

    def step(r, sums):
        row = filtered_row(planes, kernel, r)
        filtered[r] = row
        return sums[0] + folded(row), sums[1] + folded(row * row)

    sums = lax.fori_loop(0, source.shape[0], step, (zero, zero))
    for i in range(2):
        moments[i : i + 1] = jnp.sum(sums[i], axis=0, keepdims=True)


def terms_kernel(source, filtered, mean, of_flat, of_rest, pad, planes):
    spread(source, pad, planes)
    tap_sums(planes, lambda r: filtered[r] - mean[...], source.shape[0], of_rest, of_flat)


def gather_kernel(pieces, source, filtered, mean, rstd, d_normed, of_normed, sums, pad, planes):
    height, width, lanes = source.shape
    spread(source, pad, planes)
    zero = jnp.zeros((8, lanes), jnp.float32)

    def step(r, carry):
        rows = pl.ds(pl.multiple_of(r * width, width), width)
        row = pieces[0, rows].astype(jnp.float32)
        for x in range(1, 4):
            row = row + pieces[x, rows].astype(jnp.float32)
        d_normed[r] = row
        centered = (filtered[r] - mean[...]) * rstd[...]
        return carry[0] + folded(row * centered), carry[1] + folded(row)

    carry = lax.fori_loop(0, height, step, (zero, zero))
    for i in range(2):
        sums[i : i + 1] = jnp.sum(carry[i], axis=0, keepdims=True)
    tap_sums(planes, lambda r: d_normed[r], height, of_normed)


def input_kernel(d_normed, filtered, cotangent, kernel, rows, d_input, field, pad, planes):
    height = d_normed.shape[0]
    mean, rstd, scaled, shift, slope = (rows[i : i + 1] for i in range(5))

    @pl.loop(0, height)
    def _(r):
        centered = (filtered[r] - mean) * rstd
        field[r] = scaled * (d_normed[r] - shift - centered * slope)

    spread(field, pad, planes)

    @pl.loop(0, height)
    def _(r):
        row = filtered_row(planes, kernel, r, reverse=True)
        d_input[r] = (cotangent[r].astype(jnp.float32) + row).astype(jnp.bfloat16)


def conv_scratch(shape):
    height, width, lanes = shape
    return (
        pltpu.VMEM((height, width + 16, lanes), jnp.float32),
        pltpu.VMEM((KS, height + 2 * REACH, width, lanes), jnp.float32),
    )


GELU_A = 0.7978845608028654
GELU_B = 0.044715
TILE = 256
DOT_ROWS = (((0,), (0,)), ((), ()))
DOT_PLAIN = (((1,), (0,)), ((), ()))
DOT_COLS = (((1,), (1,)), ((), ()))


def dot(a, b, dims):
    return lax.dot_general(a, b, dims, preferred_element_type=jnp.float32)


def kernel_call(kernel, outs, operands, flops, scalar=False, scratch=()):
    vmem = pl.BlockSpec(memory_space=pltpu.VMEM)
    specs = [vmem] * len(operands)
    if scalar:
        specs[0] = pl.BlockSpec(memory_space=pltpu.SMEM)
    return pl.pallas_call(
        kernel,
        out_shape=[jax.ShapeDtypeStruct(s, t) for s, t in outs],
        in_specs=specs,
        out_specs=[vmem] * len(outs),
        scratch_shapes=list(scratch),
        cost_estimate=pl.CostEstimate(flops=flops, bytes_accessed=8 << 20, transcendentals=0),
        compiler_params=pltpu.CompilerParams(vmem_limit_bytes=24 << 20),
    )(*operands)


def joined(pieces, start, size):
    return jnp.concatenate([pieces[k, pl.ds(start, size)] for k in range(8)], axis=1)


def up_kernel(z, w_own, w_pair, b_own, b_pair, v_own, v_pair, slope_o, slope_p, act_o, act_p, out):
    @pl.loop(0, z.shape[1] // TILE)
    def _(m):
        start = pl.multiple_of(m * TILE, TILE)
        rows = pl.ds(start, TILE)
        x = joined(z, start, TILE)
        for w, b, slope, act in ((w_own, b_own, slope_o, act_o), (w_pair, b_pair, slope_p, act_p)):
            hidden = dot(x, w[...], DOT_PLAIN) + b[...]
            square = hidden * hidden
            t = jnp.tanh(GELU_A * (hidden + GELU_B * (square * hidden)))
            half = 0.5 * (1.0 + t)
            act[rows] = (hidden * half).astype(jnp.bfloat16)
            slope[rows] = half + (0.5 * GELU_A) * hidden * (1.0 - t * t) * (
                1.0 + 3.0 * GELU_B * square
            )
        total = dot(act_o[rows], v_own[...], DOT_PLAIN) + dot(act_p[rows], v_pair[...], DOT_PLAIN)
        for k in range(8):
            out[k, rows] = total[:, k * 128 : (k + 1) * 128].astype(jnp.bfloat16)


def down_kernel(
    core, y, slope_o, slope_p, w_own, w_pair, v_own, v_pair, back_o, back_p, bias_o, bias_p, out
):
    half = slope_o.shape[0]
    bias_o[...] = jnp.zeros_like(bias_o)
    bias_p[...] = jnp.zeros_like(bias_p)

    @pl.loop(0, half // TILE)
    def _(m):
        start = pl.multiple_of(m * TILE, TILE)
        rows = pl.ds(start, TILE)
        up = joined(y, pl.multiple_of(core[0] * half + start, TILE), TILE)
        for v, slope, back, bias in (
            (v_own, slope_o, back_o, bias_o),
            (v_pair, slope_p, back_p, bias_p),
        ):
            grad = dot(up, v[...], DOT_COLS) * slope[rows]
            bias[...] += jnp.sum(grad, axis=0, keepdims=True)
            back[rows] = grad.astype(jnp.bfloat16)
        total = dot(back_o[rows], w_own[...], DOT_COLS) + dot(back_p[rows], w_pair[...], DOT_COLS)
        for k in range(8):
            out[k, rows] = total[:, k * 128 : (k + 1) * 128].astype(jnp.bfloat16)


def weight_kernel(core, z, y, back, act, out):
    half, width = back.shape
    rows = pl.ds(pl.multiple_of(core[0] * half, half), half)

    @pl.loop(0, 4)
    def _(k):
        here = pl.ds(pl.multiple_of(k * 256, 256), 256)
        x = jnp.concatenate([z[2 * k], z[2 * k + 1]], axis=1)
        up = jnp.concatenate([y[2 * k, rows], y[2 * k + 1, rows]], axis=1)
        for a, b, cols in ((x, back, pl.ds(0, width)), (up, act, pl.ds(width, width))):
            out[here, cols] = dot(a, b[...], DOT_ROWS).astype(out.dtype)


def up_pass(z, w_own, w_pair, b_own, b_pair, v_own, v_pair):
    rows, width = z.shape[1], w_own.shape[1]
    return kernel_call(
        up_kernel,
        [((rows, width), jnp.float32)] * 2
        + [((rows, width), jnp.bfloat16)] * 2
        + [(z.shape, jnp.bfloat16)],
        (z, w_own, w_pair, b_own[None], b_pair[None], v_own, v_pair),
        8 * rows * width * 1024,
    )


def down_pass(core, y, slope_o, slope_p, w_own, w_pair, v_own, v_pair):
    rows, width = slope_o.shape
    return kernel_call(
        down_kernel,
        [((rows, width), jnp.bfloat16)] * 2
        + [((1, width), jnp.float32)] * 2
        + [((8, rows, 128), jnp.bfloat16)],
        (core, y, slope_o, slope_p, w_own, w_pair, v_own, v_pair),
        8 * rows * width * 1024,
        scalar=True,
    )


def weight_pass(kind, *operands):
    rows, width = operands[3].shape
    return kernel_call(
        weight_kernel,
        [((1024, 2 * width), kind)],
        operands,
        4 * rows * width * 1024,
        scalar=True,
    )[0]


def body(
    activations,
    cotangent,
    dw_kernel,
    norm_gain,
    norm_bias,
    w_in,
    b_in,
    w_out,
    layer_scale,
    group_sizes,
):
    channels = activations.shape[3]
    row_count = activations.shape[1] * activations.shape[2]
    core = lax.axis_index("c")
    devices = lax.axis_size(DP)
    position = lax.axis_index(DP)
    groups = group_sizes.shape[0]
    group_ends = jnp.cumsum(group_sizes)
    positions = jnp.arange(devices, dtype=jnp.int32)
    labels = jnp.sum((group_ends[None, :] <= positions[:, None]).astype(jnp.int32), axis=1)
    own_group = jnp.sum((group_ends <= position).astype(jnp.int32))
    owners = (jnp.arange(groups, dtype=jnp.int32)[:, None] == labels[None, :]).astype(jnp.float32)
    member = (jnp.arange(groups, dtype=jnp.int32) == own_group).astype(jnp.float32)
    own_count = jnp.sum(member * group_sizes.astype(jnp.float32)) * row_count
    own_gain = jnp.sum(member[:, None] * norm_gain, axis=0)
    own_bias = jnp.sum(member[:, None] * norm_bias, axis=0)

    incoming = cotangent.reshape(row_count, channels).astype(jnp.float32)
    d_branch = (incoming * layer_scale).astype(jnp.bfloat16)
    everyone = lax.all_gather(d_branch, CH, axis=0, tiled=False)
    w_in_pair = lax.ppermute(w_in, "c", SWAP)
    w_out_pair = lax.ppermute(w_out, "c", SWAP)
    b_in_pair = lax.ppermute(b_in, "c", SWAP)

    image = activations.shape[1:]
    source = activations[0]
    scratch = conv_scratch(image)
    filtered, moments = kernel_call(
        filter_kernel,
        [(image, jnp.float32), ((2, channels), jnp.float32)],
        (source, dw_kernel),
        1 << 29,
        scratch=scratch,
    )
    per_device = sent_to_all(moments, DP)
    counts = group_sizes.astype(jnp.float32)[:, None] * row_count
    totals = jnp.sum(owners[:, :, None, None] * per_device[None], axis=1)
    group_mean = totals[:, 0] / counts
    group_rstd = lax.rsqrt(totals[:, 1] / counts - group_mean * group_mean + EPS)
    own_mean = jnp.sum(member[:, None] * group_mean, axis=0)
    own_rstd = jnp.sum(member[:, None] * group_rstd, axis=0)
    centered = (filtered.reshape(row_count, channels) - own_mean) * own_rstd
    normed = (centered * own_gain + own_bias).astype(jnp.bfloat16)
    gathered = rows_of_all(normed)

    slope_own, slope_pair, active_own, active_pair, partial_branch = up_pass(
        gathered, w_in, w_in_pair, b_in, b_in_pair, w_out, w_out_pair
    )
    branch_pieces = exchanged(partial_branch)
    branch = summed(branch_pieces)
    initial = activations.reshape(row_count, channels).astype(jnp.float32)
    result = (initial + layer_scale * branch).astype(jnp.bfloat16).reshape(activations.shape)
    scale_local = jnp.sum(incoming * branch, axis=0)

    where = core.astype(jnp.int32)[None]
    back_own, back_pair, bias_own, bias_pair, partial_normed = down_pass(
        where, everyone, slope_own, slope_pair, w_in, w_in_pair, w_out, w_out_pair
    )
    for_pair = weight_pass(jnp.bfloat16, where, gathered, everyone, back_pair, active_pair)
    from_pair = lax.ppermute(for_pair, "c", SWAP)
    own_grads = weight_pass(jnp.float32, where, gathered, everyone, back_own, active_own)
    both_local = (own_grads + from_pair.astype(jnp.float32)).astype(jnp.bfloat16)
    hidden_cols = w_in.shape[1]
    bias_local = bias_own + lax.ppermute(bias_pair, "c", SWAP)
    image_mean = moments[:1] / row_count
    of_flat, of_rest = kernel_call(
        terms_kernel,
        [((64, channels), jnp.float32)] * 2,
        (source, filtered, image_mean),
        1 << 29,
        scratch=scratch,
    )
    partial_normed, branch_pieces, both_local = lax.optimization_barrier(
        (partial_normed, branch_pieces, both_local)
    )
    near = lax.psum_scatter(both_local, "z", scatter_dimension=0, tiled=True)
    normed_pieces = exchanged(partial_normed)

    from_mean = per_device[:, 0] / row_count - jnp.sum(
        owners[:, :, None] * group_mean[:, None], axis=0
    )
    normed_pieces, of_flat, of_rest = lax.optimization_barrier((normed_pieces, of_flat, of_rest))
    d_normed, of_normed, grad_moments = kernel_call(
        gather_kernel,
        [(image, jnp.float32), ((64, channels), jnp.float32), ((2, channels), jnp.float32)],
        (normed_pieces, source, filtered, own_mean[None], own_rstd[None]),
        1 << 29,
        scratch=scratch,
    )
    own_scaled = own_gain * own_rstd
    others = jnp.concatenate(
        [bias_local.reshape(4, channels), scale_local[None], jnp.zeros((64 - TAPS - 5, channels))]
    )
    firsts = jnp.concatenate([own_scaled * of_normed[:TAPS], others])
    local = jnp.stack([a.reshape(devices, 2, channels) for a in (firsts, of_flat, of_rest)], axis=1)
    sent = jnp.concatenate(
        [
            local.reshape(devices, 6, channels),
            jnp.broadcast_to(grad_moments[None], (devices, 2, channels)),
        ],
        axis=1,
    )
    parts = lax.all_to_all(sent, DP, 0, 0, tiled=True)
    grad_totals = jnp.sum(owners[:, :, None, None] * parts[None, :, 6:], axis=1)
    d_gain = grad_totals[:, 0]
    d_bias = grad_totals[:, 1]
    from_mean = per_device[:, 0] / row_count - jnp.sum(
        owners[:, :, None] * group_mean[:, None], axis=0
    )
    rest_parts = parts[:, 4:6] + from_mean[:, None] * parts[:, 2:4]
    scaled_all = norm_gain * group_rstd / counts
    flat_weight = jnp.sum(owners[:, :, None] * (scaled_all * d_bias)[:, None], axis=0)
    rest_weight = jnp.sum(
        owners[:, :, None] * (scaled_all * group_rstd * d_gain)[:, None], axis=0
    )
    piece = jnp.sum(
        parts[:, :2]
        - flat_weight[:, None] * parts[:, 2:4]
        - rest_weight[:, None] * rest_parts,
        axis=0,
    )
    total = sent_to_all(piece, DP).reshape(64, channels)
    near, total = lax.optimization_barrier((near, total))
    d_kernel = total[:TAPS]
    d_b_in = total[TAPS : TAPS + 4].ravel()
    d_scale = total[TAPS + 4]
    own_dgain = jnp.sum(member[:, None] * d_gain, axis=0)
    own_dbias = jnp.sum(member[:, None] * d_bias, axis=0)
    rows = jnp.stack(
        [own_mean, own_rstd, own_scaled, own_dbias / own_count, own_dgain / own_count]
    )
    everything = lax.all_to_all(near.reshape(4, -1, near.shape[1]), "y", 0, 0, tiled=True)
    both_sums = jnp.sum(everything.astype(jnp.float32), axis=0)
    d_w_in = both_sums[:, :hidden_cols]
    d_w_out = both_sums[:, hidden_cols:].T
    (d_input,) = kernel_call(
        input_kernel,
        [(image, jnp.bfloat16)],
        (d_normed, filtered, cotangent[0], dw_kernel, rows),
        1 << 29,
        scratch=(pltpu.VMEM(image, jnp.float32), *scratch),
    )
    d_input = d_input[None]
    return (result, d_input, d_kernel, d_gain, d_bias, d_w_in, d_b_in, d_w_out, d_scale)


def solution(mesh):
    split = Mesh(mesh.devices.reshape(8, 4, 4, 2), ("z", "y", "x", "c"))
    in_specs = (
        P(DP, None, None, CH),
        P(DP, None, None, CH),
        P(None, CH),
        P(None, CH),
        P(None, CH),
        P(None, CH),
        P(CH),
        P(CH, None),
        P(CH),
        P(),
    )
    out_specs = (
        P(DP, None, None, CH),
        P(DP, None, None, CH),
        P(None, CH),
        P(None, CH),
        P(None, CH),
        P(DP, CH),
        P(CH),
        P(CH, DP),
        P(CH),
    )
    return jax.shard_map(body, mesh=split, in_specs=in_specs, out_specs=out_specs, check_vma=False)
```

```python
import jax
import jax.numpy as jnp
from jax import lax
from jax.experimental import pallas as pl
from jax.experimental.pallas import tpu as pltpu
from jax.sharding import Mesh
from jax.sharding import PartitionSpec as P


KS = 7
DP = ("z", "y")
CH = ("x", "c")
SWAP = [(0, 1), (1, 0)]
EPS = 1e-05


def sent_to_all(array, axis):
    size = lax.axis_size(axis)
    return lax.all_to_all(
        jnp.broadcast_to(array[None], (size, *array.shape)), axis, 0, 0, tiled=True
    )


def rows_of_all(array):
    rows, own = array.shape
    halves = jnp.broadcast_to(array.reshape(1, 2, rows // 2, own), (4, 2, rows // 2, own))
    return lax.all_to_all(halves.reshape(8, rows // 2, own), CH, 0, 0, tiled=True)


def ring_scattered(array):
    here = lax.axis_index("x")
    up = [(i, (i + 1) % 4) for i in range(4)]
    down = [(i, (i + 3) % 4) for i in range(4)]

    def piece(k):
        return lax.dynamic_index_in_dim(array, (here + k) % 4, 0, keepdims=False)

    def added(a, b):
        return (a.astype(jnp.float32) + b.astype(jnp.float32)).astype(array.dtype)

    after, across, before = piece(1), piece(2), piece(3)
    cut = across.shape[1] // 2
    from_below = lax.ppermute(across[:, :cut], "x", up)
    from_above = lax.ppermute(across[:, cut:], "x", down)
    after = jnp.concatenate([added(after[:, :cut], from_below), after[:, cut:]], axis=1)
    before = jnp.concatenate([before[:, :cut], added(before[:, cut:], from_above)], axis=1)
    from_below = lax.ppermute(after, "x", up)
    from_above = lax.ppermute(before, "x", down)
    return (
        piece(0).astype(jnp.float32)
        + from_below.astype(jnp.float32)
        + from_above.astype(jnp.float32)
    )


REACH = KS // 2
TAPS = KS * KS


def spread(field, pad, planes):
    height, width, lanes = field.shape
    pad[:, :8] = jnp.zeros((height, 8, lanes), jnp.float32)
    pad[:, width + 8 :] = jnp.zeros((height, 8, lanes), jnp.float32)
    edge = jnp.zeros((KS, REACH, width, lanes), jnp.float32)
    planes[:, :REACH] = edge
    planes[:, height + REACH :] = edge

    @pl.loop(0, height)
    def _(r):
        pad[r, 8 : width + 8] = field[r].astype(jnp.float32)
        for b in range(KS):
            planes[b, r + REACH] = pad[r, 8 - REACH + b : 8 - REACH + b + width]


def filtered_row(planes, kernel, r, reverse=False):
    total = None
    for a in range(KS):
        for b in range(KS):
            tap = a * KS + b
            tap = TAPS - 1 - tap if reverse else tap
            term = planes[b, r + a] * kernel[tap : tap + 1]
            total = term if total is None else total + term
    return total


def folded(value):
    return jnp.sum(value.reshape(-1, 8, value.shape[-1]), axis=0)


def tap_sums(planes, upstream, height, out, plain=None):
    out[...] = jnp.zeros_like(out)
    if plain is not None:
        plain[...] = jnp.zeros_like(plain)
    zero = jnp.zeros((8, out.shape[1]), jnp.float32)
    for b in range(KS):

        def step(r, sums):
            u = upstream(r)
            sums = list(sums)
            for a in range(KS):
                window = planes[b, r + a]
                sums[a] = sums[a] + folded(window * u)
                if plain is not None:
                    sums[KS + a] = sums[KS + a] + folded(window)
            return tuple(sums)

        sums = lax.fori_loop(0, height, step, (zero,) * (KS if plain is None else 2 * KS))
        for a in range(KS):
            tap = a * KS + b
            out[tap : tap + 1] = jnp.sum(sums[a], axis=0, keepdims=True)
            if plain is not None:
                plain[tap : tap + 1] = jnp.sum(sums[KS + a], axis=0, keepdims=True)


def filter_kernel(*refs):
    filtered, moments, d_branch, pad, planes = refs[4:9]
    source, cotangent, scale, kernel = refs[9:13]
    copies = [
        pltpu.make_async_copy(refs[i], refs[9 + i], refs[13].at[i]) for i in range(4)
    ]
    for copy in copies:
        copy.start()
    for copy in copies:
        copy.wait()
    spread(source, pad, planes)
    zero = jnp.zeros((8, kernel.shape[1]), jnp.float32)

    def step(r, sums):
        row = filtered_row(planes, kernel, r)
        filtered[r] = row
        d_branch[r] = (cotangent[r].astype(jnp.float32) * scale[...]).astype(jnp.bfloat16)
        return sums[0] + folded(row), sums[1] + folded(row * row)

    sums = lax.fori_loop(0, source.shape[0], step, (zero, zero))
    for i in range(2):
        moments[i : i + 1] = jnp.sum(sums[i], axis=0, keepdims=True)


def terms_kernel(source, filtered, mean, of_flat, of_rest, pad, planes):
    spread(source, pad, planes)
    tap_sums(planes, lambda r: filtered[r] - mean[...], source.shape[0], of_rest, of_flat)


def gather_kernel(
    pieces, source, filtered, mean, rstd, scale, d_normed, of_normed, sums, pad, planes
):
    height, width, lanes = source.shape
    spread(source, pad, planes)
    zero = jnp.zeros((8, lanes), jnp.float32)

    def step(r, carry):
        side = r // (height // 2)
        rows = pl.ds(pl.multiple_of((r - side * (height // 2)) * width, width), width)
        row = pieces[side, rows].astype(jnp.float32)
        for x in range(1, 4):
            row = row + pieces[2 * x + side, rows].astype(jnp.float32)
        d_normed[r] = row
        centered = (filtered[r] - mean[...]) * rstd[...]
        return carry[0] + folded(row * centered), carry[1] + folded(row)

    carry = lax.fori_loop(0, height, step, (zero, zero))
    for i in range(2):
        sums[i : i + 1] = jnp.sum(carry[i], axis=0, keepdims=True)
    tail = pieces[0, pl.ds(height * width // 2, 16)].astype(jnp.float32)
    for k in range(1, 8):
        tail = tail + pieces[k, pl.ds(height * width // 2, 16)].astype(jnp.float32)
    sums[2:3] = jnp.sum(tail, axis=0, keepdims=True) / scale[...]
    tap_sums(planes, lambda r: d_normed[r], height, of_normed)


def input_kernel(d_normed, filtered, cotangent, kernel, rows, d_input, field, pad, planes):
    height = d_normed.shape[0]
    mean, rstd, scaled, shift, slope = (rows[i : i + 1] for i in range(5))

    @pl.loop(0, height)
    def _(r):
        centered = (filtered[r] - mean) * rstd
        field[r] = scaled * (d_normed[r] - shift - centered * slope)

    spread(field, pad, planes)

    @pl.loop(0, height)
    def _(r):
        row = filtered_row(planes, kernel, r, reverse=True)
        d_input[r] = (cotangent[r].astype(jnp.float32) + row).astype(jnp.bfloat16)


def conv_scratch(shape):
    height, width, lanes = shape
    return (
        pltpu.VMEM((height, width + 16, lanes), jnp.float32),
        pltpu.VMEM((KS, height + 2 * REACH, width, lanes), jnp.float32),
    )


GELU_A = 0.7978845608028654
GELU_B = 0.044715
TILE = 256
DOT_ROWS = (((0,), (0,)), ((), ()))
DOT_PLAIN = (((1,), (0,)), ((), ()))
DOT_COLS = (((1,), (1,)), ((), ()))


def dot(a, b, dims):
    return lax.dot_general(a, b, dims, preferred_element_type=jnp.float32)


def in_hbm(array):
    return pltpu.with_memory_space_constraint(array, pltpu.HBM)


def kernel_call(kernel, outs, operands, flops, scalar=False, scratch=(), space=pltpu.VMEM):
    vmem = pl.BlockSpec(memory_space=pltpu.VMEM)
    specs = [pl.BlockSpec(memory_space=space)] * len(operands)
    if scalar:
        specs[0] = pl.BlockSpec(memory_space=pltpu.SMEM)
    return pl.pallas_call(
        kernel,
        out_shape=[jax.ShapeDtypeStruct(s, t) for s, t in outs],
        in_specs=specs,
        out_specs=[vmem] * len(outs),
        scratch_shapes=list(scratch),
        cost_estimate=pl.CostEstimate(flops=flops, bytes_accessed=8 << 20, transcendentals=0),
        compiler_params=pltpu.CompilerParams(vmem_limit_bytes=24 << 20),
    )(*operands)


def joined(pieces, start, size):
    return jnp.concatenate([pieces[k, pl.ds(start, size)] for k in range(8)], axis=1)


def pointwise_kernel(core, z, y_all, w_own, w_pair, b_own, b_pair, v_own, v_pair, *rest):
    results, bias_o, bias_p, held, slopes, scale, sems = rest[:6], *rest[6:8], *rest[8:]
    act_o, act_p, back_o, back_p, out, grad_out = held[:6]
    y = held[7]
    half = z.shape[1]
    fetched = pltpu.make_async_copy(
        y_all.at[:, pl.ds(pl.multiple_of(core[0] * half, half), half)], y, sems.at[half // TILE, 1]
    )
    fetched.start()
    tiles = half // TILE
    bias_o[...] = jnp.zeros_like(bias_o)
    bias_p[...] = jnp.zeros_like(bias_p)
    scale[...] = jnp.zeros_like(scale)

    def copy(m, j):
        rows = pl.ds(pl.multiple_of(m * TILE, TILE), TILE)
        at = (slice(None), rows) if j >= 4 else (rows,)
        return pltpu.make_async_copy(held[j].at[at], results[j].at[at], sems.at[m, j])

    @pl.loop(0, tiles)
    def _(m):
        start = pl.multiple_of(m * TILE, TILE)
        rows = pl.ds(start, TILE)
        x = joined(z, start, TILE)
        for w, b, slope, act in (
            (w_own, b_own, slopes[0], act_o),
            (w_pair, b_pair, slopes[1], act_p),
        ):
            hidden = dot(x, w[...], DOT_PLAIN) + b[...]
            square = hidden * hidden
            t = jnp.tanh(GELU_A * (hidden + GELU_B * (square * hidden)))
            part = 0.5 * (1.0 + t)
            act[rows] = (hidden * part).astype(jnp.bfloat16)
            slope[...] = part + (0.5 * GELU_A) * hidden * (1.0 - t * t) * (
                1.0 + 3.0 * GELU_B * square
            )
        copy(m, 0).start()
        copy(m, 1).start()

        @pl.when(m == 0)
        def _():
            fetched.wait()

        up = joined(y, start, TILE)
        for v, slope, back, bias in (
            (v_own, slopes[0], back_o, bias_o),
            (v_pair, slopes[1], back_p, bias_p),
        ):
            grad = dot(up, v[...], DOT_COLS) * slope[...]
            bias[...] += jnp.sum(grad, axis=0, keepdims=True)
            back[rows] = grad.astype(jnp.bfloat16)
        copy(m, 2).start()
        copy(m, 3).start()
        total = dot(back_o[rows], w_own[...], DOT_COLS) + dot(back_p[rows], w_pair[...], DOT_COLS)
        for k in range(8):
            grad_out[k, rows] = total[:, k * 128 : (k + 1) * 128].astype(jnp.bfloat16)
        copy(m, 5).start()
        total = dot(act_o[rows], v_own[...], DOT_PLAIN) + dot(act_p[rows], v_pair[...], DOT_PLAIN)
        for k in range(8):
            out[k, rows] = total[:, k * 128 : (k + 1) * 128].astype(jnp.bfloat16)
        copy(m, 4).start()
        scale[...] += jnp.sum(up.astype(jnp.float32) * total, axis=0, keepdims=True)

    for k in range(8):
        value = scale[:, k * 128 : (k + 1) * 128]
        high = value.astype(jnp.bfloat16).astype(jnp.float32)
        row = lax.broadcasted_iota(jnp.int32, (16, 128), 0)
        both = jnp.where(row == 0, high, jnp.where(row == 1, value - high, 0.0))
        held[6][k] = both.astype(jnp.bfloat16)
    last = pltpu.make_async_copy(
        held[6], results[5].at[:, pl.ds(half, 16)], sems.at[tiles, 0]
    )
    last.start()
    for m in range(tiles):
        for j in range(6):
            copy(m, j).wait()
    last.wait()


def weight_kernel(core, z, y, back, act, out):
    half, width = back.shape
    rows = pl.ds(pl.multiple_of(core[0] * half, half), half)

    @pl.loop(0, 4)
    def _(k):
        here = pl.ds(pl.multiple_of(k * 256, 256), 256)
        x = jnp.concatenate([z[2 * k], z[2 * k + 1]], axis=1)
        up = jnp.concatenate([y[2 * k, rows], y[2 * k + 1, rows]], axis=1)
        for a, b, cols in ((x, back, pl.ds(0, width)), (up, act, pl.ds(width, width))):
            out[here, cols] = dot(a, b[...], DOT_ROWS).astype(out.dtype)


def pointwise_pass(core, z, y, w_own, w_pair, b_own, b_pair, v_own, v_pair):
    rows, width = z.shape[1], w_own.shape[1]
    vmem = pl.BlockSpec(memory_space=pltpu.VMEM)
    flat, wide = (rows, width), (8, rows, 128)
    outs = [flat] * 4 + [wide, (8, rows + 16, 128)]
    held = tuple(pltpu.VMEM(s, jnp.bfloat16) for s in [flat] * 4 + [wide, wide, (8, 16, 128), wide])
    return pl.pallas_call(
        lambda *refs: pointwise_kernel(*refs[:17], refs[17:25], refs[25:27], *refs[27:]),
        out_shape=[pltpu.HBM(s, jnp.bfloat16) for s in outs]
        + [jax.ShapeDtypeStruct((1, width), jnp.float32)] * 2,
        in_specs=[pl.BlockSpec(memory_space=pltpu.SMEM), vmem]
        + [pl.BlockSpec(memory_space=pltpu.HBM)]
        + [vmem] * 6,
        out_specs=[pl.BlockSpec(memory_space=pltpu.HBM)] * 6 + [vmem] * 2,
        scratch_shapes=[
            *held,
            pltpu.VMEM((TILE, width), jnp.float32),
            pltpu.VMEM((TILE, width), jnp.float32),
            pltpu.VMEM((1, 1024), jnp.float32),
            pltpu.SemaphoreType.DMA((rows // TILE + 1, 6)),
        ],
        cost_estimate=pl.CostEstimate(
            flops=16 * rows * width * 1024, bytes_accessed=8 << 20, transcendentals=0
        ),
        compiler_params=pltpu.CompilerParams(vmem_limit_bytes=36 << 20),
    )(core, z, in_hbm(y), w_own, w_pair, b_own[None], b_pair[None], v_own, v_pair)


def weight_pass(kind, *operands):
    rows, width = operands[3].shape
    return kernel_call(
        weight_kernel,
        [((1024, 2 * width), kind)],
        operands,
        4 * rows * width * 1024,
        scalar=True,
    )[0]


def body(
    activations,
    cotangent,
    dw_kernel,
    norm_gain,
    norm_bias,
    w_in,
    b_in,
    w_out,
    layer_scale,
    group_sizes,
):
    channels = activations.shape[3]
    row_count = activations.shape[1] * activations.shape[2]
    core = lax.axis_index("c")
    devices = lax.axis_size(DP)
    position = lax.axis_index(DP)
    groups = group_sizes.shape[0]
    group_ends = jnp.cumsum(group_sizes)
    positions = jnp.arange(devices, dtype=jnp.int32)
    labels = jnp.sum((group_ends[None, :] <= positions[:, None]).astype(jnp.int32), axis=1)
    own_group = jnp.sum((group_ends <= position).astype(jnp.int32))
    owners = (jnp.arange(groups, dtype=jnp.int32)[:, None] == labels[None, :]).astype(jnp.float32)
    member = (jnp.arange(groups, dtype=jnp.int32) == own_group).astype(jnp.float32)
    own_count = jnp.sum(member * group_sizes.astype(jnp.float32)) * row_count
    own_gain = jnp.sum(member[:, None] * norm_gain, axis=0)
    own_bias = jnp.sum(member[:, None] * norm_bias, axis=0)

    w_in_pair = lax.ppermute(w_in, "c", SWAP)
    w_out_pair = lax.ppermute(w_out, "c", SWAP)
    b_in_pair = lax.ppermute(b_in, "c", SWAP)

    image = activations.shape[1:]
    source = activations[0]
    scratch = conv_scratch(image)
    operands = (source, cotangent[0], layer_scale[None], dw_kernel)
    filtered, moments, d_branch = kernel_call(
        filter_kernel,
        [(image, jnp.float32), ((2, channels), jnp.float32), (image, jnp.bfloat16)],
        tuple(in_hbm(a) for a in operands),
        1 << 29,
        scratch=(
            *scratch,
            *(pltpu.VMEM(a.shape, a.dtype) for a in operands),
            pltpu.SemaphoreType.DMA((4,)),
        ),
        space=pltpu.HBM,
    )
    everyone = lax.all_gather(d_branch.reshape(row_count, channels), CH)
    per_device = sent_to_all(moments, DP)
    counts = group_sizes.astype(jnp.float32)[:, None] * row_count
    totals = jnp.sum(owners[:, :, None, None] * per_device[None], axis=1)
    group_mean = totals[:, 0] / counts
    group_rstd = lax.rsqrt(totals[:, 1] / counts - group_mean * group_mean + EPS)
    own_mean = jnp.sum(member[:, None] * group_mean, axis=0)
    own_rstd = jnp.sum(member[:, None] * group_rstd, axis=0)
    centered = (filtered.reshape(row_count, channels) - own_mean) * own_rstd
    normed = (centered * own_gain + own_bias).astype(jnp.bfloat16)
    image_mean = moments[:1] / row_count
    of_flat, of_rest = kernel_call(
        terms_kernel,
        [((64, channels), jnp.float32)] * 2,
        (source, filtered, image_mean),
        1 << 29,
        scratch=scratch,
    )
    gathered = rows_of_all(normed)
    gathered, of_flat, of_rest = lax.optimization_barrier((gathered, of_flat, of_rest))

    where = core.astype(jnp.int32)[None]
    (
        active_own,
        active_pair,
        back_own,
        back_pair,
        partial_branch,
        partial_normed,
        bias_own,
        bias_pair,
    ) = pointwise_pass(where, gathered, everyone, w_in, w_in_pair, b_in, b_in_pair, w_out, w_out_pair)
    normed_pieces = lax.all_to_all(partial_normed, CH, 0, 0, tiled=True)
    for_pair = weight_pass(jnp.bfloat16, where, gathered, everyone, back_pair, active_pair)
    from_pair = lax.ppermute(for_pair, "c", SWAP)
    own_grads = weight_pass(jnp.float32, where, gathered, everyone, back_own, active_own)
    both_local = (own_grads + from_pair.astype(jnp.float32)).astype(jnp.bfloat16)
    hidden_cols = w_in.shape[1]
    bias_local = bias_own + lax.ppermute(bias_pair, "c", SWAP)
    near = lax.psum_scatter(both_local, "z", scatter_dimension=0, tiled=True)

    from_mean = per_device[:, 0] / row_count - jnp.sum(
        owners[:, :, None] * group_mean[:, None], axis=0
    )
    d_normed, of_normed, grad_moments = kernel_call(
        gather_kernel,
        [(image, jnp.float32), ((64, channels), jnp.float32), ((3, channels), jnp.float32)],
        (normed_pieces, source, filtered, own_mean[None], own_rstd[None], layer_scale[None]),
        1 << 29,
        scratch=scratch,
    )
    own_scaled = own_gain * own_rstd
    others = jnp.concatenate(
        [bias_local.reshape(4, channels), grad_moments[2:], jnp.zeros((64 - TAPS - 5, channels))]
    )
    firsts = jnp.concatenate([own_scaled * of_normed[:TAPS], others])
    local = jnp.stack([a.reshape(devices, 2, channels) for a in (firsts, of_flat, of_rest)], axis=1)
    sent = jnp.concatenate(
        [
            local.reshape(devices, 6, channels),
            jnp.broadcast_to(grad_moments[None, :2], (devices, 2, channels)),
        ],
        axis=1,
    )
    sent, partial_branch = lax.optimization_barrier((sent, partial_branch))
    parts = lax.all_to_all(sent, DP, 0, 0, tiled=True)
    halves = (4, 2, row_count // 2, channels)
    chip_branch = ring_scattered(partial_branch.reshape(halves)).astype(jnp.bfloat16)
    kept = lax.dynamic_index_in_dim(chip_branch, core, 0, keepdims=False)
    given = lax.dynamic_index_in_dim(chip_branch, 1 - core, 0, keepdims=False)
    taken = lax.ppermute(given, "c", SWAP)
    branch = jnp.concatenate(
        [jnp.where(core == 0, kept, taken), jnp.where(core == 0, taken, kept)]
    ).astype(jnp.float32)
    initial = activations.reshape(row_count, channels).astype(jnp.float32)
    result = (initial + layer_scale * branch).astype(jnp.bfloat16).reshape(activations.shape)
    grad_totals = jnp.sum(owners[:, :, None, None] * parts[None, :, 6:], axis=1)
    d_gain = grad_totals[:, 0]
    d_bias = grad_totals[:, 1]
    from_mean = per_device[:, 0] / row_count - jnp.sum(
        owners[:, :, None] * group_mean[:, None], axis=0
    )
    rest_parts = parts[:, 4:6] + from_mean[:, None] * parts[:, 2:4]
    scaled_all = norm_gain * group_rstd / counts
    flat_weight = jnp.sum(owners[:, :, None] * (scaled_all * d_bias)[:, None], axis=0)
    rest_weight = jnp.sum(
        owners[:, :, None] * (scaled_all * group_rstd * d_gain)[:, None], axis=0
    )
    piece = jnp.sum(
        parts[:, :2]
        - flat_weight[:, None] * parts[:, 2:4]
        - rest_weight[:, None] * rest_parts,
        axis=0,
    )
    total = sent_to_all(piece, DP).reshape(64, channels)
    near, total = lax.optimization_barrier((near, total))
    d_kernel = total[:TAPS]
    d_b_in = total[TAPS : TAPS + 4].ravel()
    d_scale = total[TAPS + 4]
    own_dgain = jnp.sum(member[:, None] * d_gain, axis=0)
    own_dbias = jnp.sum(member[:, None] * d_bias, axis=0)
    rows = jnp.stack(
        [own_mean, own_rstd, own_scaled, own_dbias / own_count, own_dgain / own_count]
    )
    everything = lax.all_to_all(near.reshape(4, -1, near.shape[1]), "y", 0, 0, tiled=True)
    both_sums = jnp.sum(everything.astype(jnp.float32), axis=0)
    d_w_in = both_sums[:, :hidden_cols]
    d_w_out = both_sums[:, hidden_cols:].T
    (d_input,) = kernel_call(
        input_kernel,
        [(image, jnp.bfloat16)],
        (d_normed, filtered, cotangent[0], dw_kernel, rows),
        1 << 29,
        scratch=(pltpu.VMEM(image, jnp.float32), *scratch),
    )
    d_input = d_input[None]
    return (result, d_input, d_kernel, d_gain, d_bias, d_w_in, d_b_in, d_w_out, d_scale)


def solution(mesh):
    split = Mesh(mesh.devices.reshape(8, 4, 4, 2), ("z", "y", "x", "c"))
    in_specs = (
        P(DP, None, None, CH),
        P(DP, None, None, CH),
        P(None, CH),
        P(None, CH),
        P(None, CH),
        P(None, CH),
        P(CH),
        P(CH, None),
        P(CH),
        P(),
    )
    out_specs = (
        P(DP, None, None, CH),
        P(DP, None, None, CH),
        P(None, CH),
        P(None, CH),
        P(None, CH),
        P(DP, CH),
        P(CH),
        P(CH, DP),
        P(CH),
    )
    return jax.shard_map(body, mesh=split, in_specs=in_specs, out_specs=out_specs, check_vma=False)
```

```python
import jax
import jax.numpy as jnp
from jax import lax
from jax.experimental import pallas as pl
from jax.experimental.pallas import tpu as pltpu
from jax.sharding import Mesh
from jax.sharding import PartitionSpec as P


KS = 7
DP = ("z", "y")
CH = ("x", "c")
SWAP = [(0, 1), (1, 0)]
EPS = 1e-05


def sent_to_all(array, axis):
    size = lax.axis_size(axis)
    return lax.all_to_all(
        jnp.broadcast_to(array[None], (size, *array.shape)), axis, 0, 0, tiled=True
    )


def rows_of_all(array):
    rows, own = array.shape
    halves = jnp.broadcast_to(array.reshape(1, 2, rows // 2, own), (4, 2, rows // 2, own))
    return lax.all_to_all(halves.reshape(8, rows // 2, own), CH, 0, 0, tiled=True)


def ring_scattered(array, axis):
    here = lax.axis_index(axis)

    def piece(k):
        return lax.dynamic_index_in_dim(array, (here + k) % 4, 0, keepdims=False)

    terms = [piece(0)] + [
        lax.ppermute(piece(k), axis, [(i, (i + k) % 4) for i in range(4)]) for k in (2, 1, 3)
    ]
    return sum(term.astype(jnp.float32) for term in terms)


REACH = KS // 2
TAPS = KS * KS


def spread(field, pad, planes):
    height, width, lanes = field.shape
    pad[:, :8] = jnp.zeros((height, 8, lanes), jnp.float32)
    pad[:, width + 8 :] = jnp.zeros((height, 8, lanes), jnp.float32)
    edge = jnp.zeros((KS, REACH, width, lanes), jnp.float32)
    planes[:, :REACH] = edge
    planes[:, height + REACH :] = edge

    @pl.loop(0, height)
    def _(r):
        pad[r, 8 : width + 8] = field[r].astype(jnp.float32)
        for b in range(KS):
            planes[b, r + REACH] = pad[r, 8 - REACH + b : 8 - REACH + b + width]


BLOCK = 4


def filtered_rows(planes, kernel, start, reverse=False):
    totals = [None] * BLOCK
    for b in range(KS):
        for t in range(BLOCK + KS - 1):
            window = planes[b, start + t]
            for i in range(BLOCK):
                if 0 <= t - i < KS:
                    tap = (t - i) * KS + b
                    tap = TAPS - 1 - tap if reverse else tap
                    term = window * kernel[tap : tap + 1]
                    totals[i] = term if totals[i] is None else totals[i] + term
    return totals


def folded(value):
    return jnp.sum(value.reshape(-1, 8, value.shape[-1]), axis=0)


def tap_sums(planes, upstream, height, width, store, plain=None):
    zero = jnp.zeros((8, planes.shape[-1]), jnp.float32)
    for b in range(KS):

        def step(block, sums):
            start = block * BLOCK
            sums = list(sums)
            for j in range(width // 8):
                cols = pl.ds(8 * j, 8)
                ups = [upstream(start + i, cols) for i in range(BLOCK)]
                for t in range(BLOCK + KS - 1):
                    window = planes[b, start + t, cols]
                    for i in range(BLOCK):
                        if 0 <= t - i < KS:
                            sums[t - i] = sums[t - i] + window * ups[i]
                            if plain is not None:
                                sums[KS + t - i] = sums[KS + t - i] + window
            return tuple(sums)

        count = KS if plain is None else 2 * KS
        sums = lax.fori_loop(0, height // BLOCK, step, (zero,) * count)
        for a in range(KS):
            store(a * KS + b, jnp.sum(sums[a], axis=0, keepdims=True))
            if plain is not None:
                plain(a * KS + b, jnp.sum(sums[KS + a], axis=0, keepdims=True))


def row_store(ref, first):
    def store(tap, row):
        ref[tap // 2, pl.ds(first + tap % 2, 1)] = row

    return store


def filter_kernel(*refs):
    filtered, moments, d_branch, pad, planes = refs[4:9]
    source, cotangent, scale, kernel = refs[9:13]
    copies = [
        pltpu.make_async_copy(refs[i], refs[9 + i], refs[13].at[i]) for i in range(4)
    ]
    for copy in copies:
        copy.start()
    for copy in copies:
        copy.wait()
    spread(source, pad, planes)
    zero = jnp.zeros((8, kernel.shape[1]), jnp.float32)

    def step(block, sums):
        start = block * BLOCK
        first, second = sums
        for i, row in enumerate(filtered_rows(planes, kernel, start)):
            r = start + i
            filtered[r] = row
            d_branch[r] = (cotangent[r].astype(jnp.float32) * scale[...]).astype(jnp.bfloat16)
            first, second = first + folded(row), second + folded(row * row)
        return first, second

    sums = lax.fori_loop(0, source.shape[0] // BLOCK, step, (zero, zero))
    for i in range(2):
        row = jnp.sum(sums[i], axis=0, keepdims=True)
        moments[:, i : i + 1] = jnp.broadcast_to(row[None], (moments.shape[0], *row.shape))


def terms_kernel(source, filtered, mean, sent, pad, planes):
    height, width, _ = source.shape
    sent[...] = jnp.zeros_like(sent)
    spread(source, pad, planes)
    tap_sums(
        planes,
        lambda r, cols: filtered[r, cols] - mean[...],
        height,
        width,
        row_store(sent, 4),
        row_store(sent, 2),
    )


def gather_kernel(
    pieces, source, filtered, rows, bias, base, d_normed, sent, pad, planes
):
    height, width, lanes = source.shape
    mean, rstd, scale, scaled = (rows[i : i + 1] for i in range(4))
    sent[...] = base[...]
    spread(source, pad, planes)
    zero = jnp.zeros((8, lanes), jnp.float32)

    def step(r, carry):
        side = r // (height // 2)
        here = pl.ds(pl.multiple_of((r - side * (height // 2)) * width, width), width)
        row = pieces[side, here].astype(jnp.float32)
        for x in range(1, 4):
            row = row + pieces[2 * x + side, here].astype(jnp.float32)
        d_normed[r] = row
        centered = (filtered[r] - mean) * rstd
        return carry[0] + folded(row * centered), carry[1] + folded(row)

    carry = lax.fori_loop(0, height, step, (zero, zero))
    for i in range(2):
        row = jnp.sum(carry[i], axis=0, keepdims=True)
        sent[:, 6 + i : 7 + i] = jnp.broadcast_to(row[None], (sent.shape[0], 1, lanes))
    tail = pieces[0, pl.ds(height * width // 2, 16)].astype(jnp.float32)
    for k in range(1, 8):
        tail = tail + pieces[k, pl.ds(height * width // 2, 16)].astype(jnp.float32)
    store = row_store(sent, 0)
    for q in range(4):
        store(TAPS + q, bias[:, q * lanes : (q + 1) * lanes])
    store(TAPS + 4, jnp.sum(tail, axis=0, keepdims=True) / scale)
    tap_sums(
        planes,
        lambda r, cols: d_normed[r, cols],
        height,
        width,
        lambda tap, row: store(tap, scaled * row),
    )


def input_kernel(d_normed, filtered, cotangent, kernel, rows, d_input, field, pad, planes):
    height = d_normed.shape[0]
    mean, rstd, scaled, shift, slope = (rows[i : i + 1] for i in range(5))

    @pl.loop(0, height)
    def _(r):
        centered = (filtered[r] - mean) * rstd
        field[r] = scaled * (d_normed[r] - shift - centered * slope)

    spread(field, pad, planes)

    @pl.loop(0, height // BLOCK)
    def _(block):
        start = block * BLOCK
        for i, row in enumerate(filtered_rows(planes, kernel, start, reverse=True)):
            r = start + i
            d_input[r] = (cotangent[r].astype(jnp.float32) + row).astype(jnp.bfloat16)


def conv_scratch(shape):
    height, width, lanes = shape
    return (
        pltpu.VMEM((height, width + 16, lanes), jnp.float32),
        pltpu.VMEM((KS, height + 2 * REACH, width, lanes), jnp.float32),
    )


GELU_A = 0.7978845608028654
GELU_B = 0.044715
TILE = 256
DOT_ROWS = (((0,), (0,)), ((), ()))
DOT_PLAIN = (((1,), (0,)), ((), ()))
DOT_COLS = (((1,), (1,)), ((), ()))


def dot(a, b, dims):
    return lax.dot_general(a, b, dims, preferred_element_type=jnp.float32)


def in_hbm(array):
    return pltpu.with_memory_space_constraint(array, pltpu.HBM)


def kernel_call(kernel, outs, operands, flops, scalar=False, scratch=(), space=pltpu.VMEM):
    vmem = pl.BlockSpec(memory_space=pltpu.VMEM)
    specs = [pl.BlockSpec(memory_space=space)] * len(operands)
    if scalar:
        specs[0] = pl.BlockSpec(memory_space=pltpu.SMEM)
    return pl.pallas_call(
        kernel,
        out_shape=[jax.ShapeDtypeStruct(s, t) for s, t in outs],
        in_specs=specs,
        out_specs=[vmem] * len(outs),
        scratch_shapes=list(scratch),
        cost_estimate=pl.CostEstimate(flops=flops, bytes_accessed=8 << 20, transcendentals=0),
        compiler_params=pltpu.CompilerParams(vmem_limit_bytes=24 << 20),
    )(*operands)


def joined(pieces, start, size):
    return jnp.concatenate([pieces[k, pl.ds(start, size)] for k in range(8)], axis=1)


def pointwise_kernel(core, z, y_all, w_own, w_pair, b_own, b_pair, v_own_far, v_pair_far, *rest):
    results, rest = rest[:4], rest[4:]
    bias_o, bias_p, held, slopes, scale, v_own, v_pair, pair, own, sems = rest
    act_o, act_p, back_o, back_p, out, grad_out = held[:6]
    y = held[7]
    half = z.shape[1]
    fetched = pltpu.make_async_copy(
        y_all.at[:, pl.ds(pl.multiple_of(core[0] * half, half), half)], y, sems.at[half // TILE, 1]
    )
    fetched = [
        fetched,
        pltpu.make_async_copy(v_own_far, v_own, sems.at[half // TILE, 2]),
        pltpu.make_async_copy(v_pair_far, v_pair, sems.at[half // TILE, 3]),
    ]
    for copy_in in fetched:
        copy_in.start()
    tiles = half // TILE
    bias_o[...] = jnp.zeros_like(bias_o)
    bias_p[...] = jnp.zeros_like(bias_p)
    scale[...] = jnp.zeros_like(scale)

    def copy(m, j):
        rows = pl.ds(pl.multiple_of(m * TILE, TILE), TILE)
        at = (slice(None), rows)
        return pltpu.make_async_copy(held[j].at[at], results[j - 4].at[at], sems.at[m, j])

    @pl.loop(0, tiles)
    def _(m):
        start = pl.multiple_of(m * TILE, TILE)
        rows = pl.ds(start, TILE)
        x = joined(z, start, TILE)
        for w, b, slope, act in (
            (w_own, b_own, slopes[0], act_o),
            (w_pair, b_pair, slopes[1], act_p),
        ):
            hidden = dot(x, w[...], DOT_PLAIN) + b[...]
            square = hidden * hidden
            t = jnp.tanh(GELU_A * (hidden + GELU_B * (square * hidden)))
            part = 0.5 * (1.0 + t)
            act[rows] = (hidden * part).astype(jnp.bfloat16)
            slope[...] = part + (0.5 * GELU_A) * hidden * (1.0 - t * t) * (
                1.0 + 3.0 * GELU_B * square
            )

        @pl.when(m == 0)
        def _():
            for copy_in in fetched:
                copy_in.wait()

        up = joined(y, start, TILE)
        for v, slope, back, bias in (
            (v_own, slopes[0], back_o, bias_o),
            (v_pair, slopes[1], back_p, bias_p),
        ):
            grad = dot(up, v[...], DOT_COLS) * slope[...]
            bias[...] += jnp.sum(grad, axis=0, keepdims=True)
            back[rows] = grad.astype(jnp.bfloat16)
        total = dot(back_o[rows], w_own[...], DOT_COLS) + dot(back_p[rows], w_pair[...], DOT_COLS)
        for k in range(8):
            grad_out[k, rows] = total[:, k * 128 : (k + 1) * 128].astype(jnp.bfloat16)
        copy(m, 5).start()
        total = dot(act_o[rows], v_own[...], DOT_PLAIN) + dot(act_p[rows], v_pair[...], DOT_PLAIN)
        for k in range(8):
            out[k, rows] = total[:, k * 128 : (k + 1) * 128].astype(jnp.bfloat16)
        copy(m, 4).start()
        scale[...] += jnp.sum(up.astype(jnp.float32) * total, axis=0, keepdims=True)

    for k in range(8):
        value = scale[:, k * 128 : (k + 1) * 128]
        high = value.astype(jnp.bfloat16).astype(jnp.float32)
        row = lax.broadcasted_iota(jnp.int32, (16, 128), 0)
        both = jnp.where(row == 0, high, jnp.where(row == 1, value - high, 0.0))
        held[6][k] = both.astype(jnp.bfloat16)
    last = pltpu.make_async_copy(
        held[6], results[1].at[:, pl.ds(half, 16)], sems.at[tiles, 0]
    )
    last.start()

    def grad_copy(k, i):
        here = pl.ds(pl.multiple_of(k * 256, 256), 256)
        grads = (pair, own)[i]
        return pltpu.make_async_copy(
            grads.at[here], results[2 + i].at[here], sems.at[tiles + 1 + i, k]
        )

    width = back_p.shape[1]
    for i, (grads, back, act) in enumerate(((pair, back_p, act_p), (own, back_o, act_o))):

        @pl.loop(0, 4)
        def _(k):
            here = pl.ds(pl.multiple_of(k * 256, 256), 256)
            x = jnp.concatenate([z[2 * k], z[2 * k + 1]], axis=1)
            up = jnp.concatenate([y[2 * k], y[2 * k + 1]], axis=1)
            grads[here, :width] = dot(x, back[...], DOT_ROWS).astype(jnp.bfloat16)
            grads[here, width:] = dot(up, act[...], DOT_ROWS).astype(jnp.bfloat16)
            grad_copy(k, i).start()

    for m in range(tiles):
        for j in (4, 5):
            copy(m, j).wait()
    last.wait()
    for i in range(2):
        for k in range(4):
            grad_copy(k, i).wait()


def pointwise_pass(core, z, y, w_own, w_pair, b_own, b_pair, v_own, v_pair):
    rows, width = z.shape[1], w_own.shape[1]
    vmem = pl.BlockSpec(memory_space=pltpu.VMEM)
    flat, wide = (rows, width), (8, rows, 128)
    outs = [wide, (8, rows + 16, 128)] + [(1024, 2 * width)] * 2
    held = tuple(pltpu.VMEM(s, jnp.bfloat16) for s in [flat] * 4 + [wide, wide, (8, 16, 128), wide])
    return pl.pallas_call(
        lambda *refs: pointwise_kernel(*refs[:15], refs[15:23], refs[23:25], *refs[25:]),
        out_shape=[pltpu.HBM(s, jnp.bfloat16) for s in outs]
        + [jax.ShapeDtypeStruct((1, width), jnp.float32)] * 2,
        in_specs=[pl.BlockSpec(memory_space=pltpu.SMEM), vmem]
        + [pl.BlockSpec(memory_space=pltpu.HBM)]
        + [vmem] * 4
        + [pl.BlockSpec(memory_space=pltpu.HBM)] * 2,
        out_specs=[pl.BlockSpec(memory_space=pltpu.HBM)] * 4 + [vmem] * 2,
        scratch_shapes=[
            *held,
            pltpu.VMEM((TILE, width), jnp.float32),
            pltpu.VMEM((TILE, width), jnp.float32),
            pltpu.VMEM((1, 1024), jnp.float32),
            pltpu.VMEM(v_own.shape, jnp.bfloat16),
            pltpu.VMEM(v_own.shape, jnp.bfloat16),
            pltpu.VMEM((1024, 2 * width), jnp.bfloat16),
            pltpu.VMEM((1024, 2 * width), jnp.bfloat16),
            pltpu.SemaphoreType.DMA((rows // TILE + 3, 6)),
        ],
        cost_estimate=pl.CostEstimate(
            flops=16 * rows * width * 1024, bytes_accessed=8 << 20, transcendentals=0
        ),
        compiler_params=pltpu.CompilerParams(vmem_limit_bytes=36 << 20),
    )(
        core,
        z,
        in_hbm(y),
        w_own,
        w_pair,
        b_own[None],
        b_pair[None],
        in_hbm(v_own),
        in_hbm(v_pair),
    )


def body(
    activations,
    cotangent,
    dw_kernel,
    norm_gain,
    norm_bias,
    w_in,
    b_in,
    w_out,
    layer_scale,
    group_sizes,
):
    channels = activations.shape[3]
    row_count = activations.shape[1] * activations.shape[2]
    core = lax.axis_index("c")
    devices = lax.axis_size(DP)
    position = lax.axis_index(DP)
    groups = group_sizes.shape[0]
    group_ends = jnp.cumsum(group_sizes)
    positions = jnp.arange(devices, dtype=jnp.int32)
    labels = jnp.sum((group_ends[None, :] <= positions[:, None]).astype(jnp.int32), axis=1)
    own_group = jnp.sum((group_ends <= position).astype(jnp.int32))
    owners = (jnp.arange(groups, dtype=jnp.int32)[:, None] == labels[None, :]).astype(jnp.float32)
    member = (jnp.arange(groups, dtype=jnp.int32) == own_group).astype(jnp.float32)
    own_count = jnp.sum(member * group_sizes.astype(jnp.float32)) * row_count
    own_gain = jnp.sum(member[:, None] * norm_gain, axis=0)
    own_bias = jnp.sum(member[:, None] * norm_bias, axis=0)

    w_in_pair = lax.ppermute(w_in, "c", SWAP)
    w_out_pair = lax.ppermute(w_out, "c", SWAP)
    b_in_pair = lax.ppermute(b_in, "c", SWAP)

    image = activations.shape[1:]
    source = activations[0]
    scratch = conv_scratch(image)
    operands = (source, cotangent[0], layer_scale[None], dw_kernel)
    filtered, moments, d_branch = kernel_call(
        filter_kernel,
        [(image, jnp.float32), ((devices, 2, channels), jnp.float32), (image, jnp.bfloat16)],
        tuple(in_hbm(a) for a in operands),
        1 << 29,
        scratch=(
            *scratch,
            *(pltpu.VMEM(a.shape, a.dtype) for a in operands),
            pltpu.SemaphoreType.DMA((4,)),
        ),
        space=pltpu.HBM,
    )
    everyone = lax.all_gather(d_branch.reshape(row_count, channels), CH)
    per_device = lax.all_to_all(moments, DP, 0, 0, tiled=True)
    counts = group_sizes.astype(jnp.float32)[:, None] * row_count
    totals = jnp.sum(owners[:, :, None, None] * per_device[None], axis=1)
    group_mean = totals[:, 0] / counts
    group_rstd = lax.rsqrt(totals[:, 1] / counts - group_mean * group_mean + EPS)
    own_mean = jnp.sum(member[:, None] * group_mean, axis=0)
    own_rstd = jnp.sum(member[:, None] * group_rstd, axis=0)
    centered = (filtered.reshape(row_count, channels) - own_mean) * own_rstd
    normed = (centered * own_gain + own_bias).astype(jnp.bfloat16)
    (base,) = kernel_call(
        terms_kernel,
        [((devices, 8, channels), jnp.float32)],
        (source, filtered, moments[0, :1] / row_count),
        1 << 29,
        scratch=scratch,
    )
    gathered = rows_of_all(normed)
    gathered, base = lax.optimization_barrier((gathered, base))

    where = core.astype(jnp.int32)[None]
    (
        partial_branch,
        partial_normed,
        for_pair,
        own_grads,
        bias_own,
        bias_pair,
    ) = pointwise_pass(where, gathered, everyone, w_in, w_in_pair, b_in, b_in_pair, w_out, w_out_pair)
    normed_pieces = lax.all_to_all(partial_normed, CH, 0, 0, tiled=True)
    from_pair = lax.ppermute(for_pair, "c", SWAP)
    both_local = own_grads.astype(jnp.float32) + from_pair.astype(jnp.float32)
    both_local = both_local.astype(jnp.bfloat16)
    hidden_cols = w_in.shape[1]
    bias_local = bias_own + lax.ppermute(bias_pair, "c", SWAP)
    near = lax.psum_scatter(both_local, "z", scatter_dimension=0, tiled=True)

    from_mean = per_device[:, 0] / row_count - jnp.sum(
        owners[:, :, None] * group_mean[:, None], axis=0
    )
    own_scaled = own_gain * own_rstd
    d_normed, sent = kernel_call(
        gather_kernel,
        [(image, jnp.float32), (base.shape, jnp.float32)],
        (
            normed_pieces,
            source,
            filtered,
            jnp.stack([own_mean, own_rstd, layer_scale, own_scaled]),
            bias_local,
            base,
        ),
        1 << 29,
        scratch=scratch,
    )
    sent, partial_branch = lax.optimization_barrier((sent, partial_branch))
    parts = lax.all_to_all(sent, DP, 0, 0, tiled=True)
    halves = (4, 2, row_count // 2, channels)
    chip_branch = ring_scattered(partial_branch.reshape(halves), "x").astype(jnp.bfloat16)
    kept = lax.dynamic_index_in_dim(chip_branch, core, 0, keepdims=False)
    given = lax.dynamic_index_in_dim(chip_branch, 1 - core, 0, keepdims=False)
    taken = lax.ppermute(given, "c", SWAP)
    branch = jnp.concatenate(
        [jnp.where(core == 0, kept, taken), jnp.where(core == 0, taken, kept)]
    ).astype(jnp.float32)
    initial = activations.reshape(row_count, channels).astype(jnp.float32)
    result = (initial + layer_scale * branch).astype(jnp.bfloat16).reshape(activations.shape)
    grad_totals = jnp.sum(owners[:, :, None, None] * parts[None, :, 6:], axis=1)
    d_gain = grad_totals[:, 0]
    d_bias = grad_totals[:, 1]
    from_mean = per_device[:, 0] / row_count - jnp.sum(
        owners[:, :, None] * group_mean[:, None], axis=0
    )
    rest_parts = parts[:, 4:6] + from_mean[:, None] * parts[:, 2:4]
    scaled_all = norm_gain * group_rstd / counts
    flat_weight = jnp.sum(owners[:, :, None] * (scaled_all * d_bias)[:, None], axis=0)
    rest_weight = jnp.sum(
        owners[:, :, None] * (scaled_all * group_rstd * d_gain)[:, None], axis=0
    )
    piece = jnp.sum(
        parts[:, :2]
        - flat_weight[:, None] * parts[:, 2:4]
        - rest_weight[:, None] * rest_parts,
        axis=0,
    )
    total = sent_to_all(piece, DP).reshape(64, channels)
    d_kernel = total[:TAPS]
    d_b_in = total[TAPS : TAPS + 4].ravel()
    d_scale = total[TAPS + 4]
    own_dgain = jnp.sum(member[:, None] * d_gain, axis=0)
    own_dbias = jnp.sum(member[:, None] * d_bias, axis=0)
    rows = jnp.stack(
        [own_mean, own_rstd, own_scaled, own_dbias / own_count, own_dgain / own_count]
    )
    (d_input,) = kernel_call(
        input_kernel,
        [(image, jnp.bfloat16)],
        (d_normed, filtered, cotangent[0], dw_kernel, rows),
        1 << 29,
        scratch=(pltpu.VMEM(image, jnp.float32), *scratch),
    )
    d_input = d_input[None]
    both_sums = ring_scattered(near.reshape(4, -1, near.shape[1]), "y")
    d_w_in = both_sums[:, :hidden_cols]
    d_w_out = both_sums[:, hidden_cols:].T
    return (result, d_input, d_kernel, d_gain, d_bias, d_w_in, d_b_in, d_w_out, d_scale)


def solution(mesh):
    split = Mesh(mesh.devices.reshape(8, 4, 4, 2), ("z", "y", "x", "c"))
    in_specs = (
        P(DP, None, None, CH),
        P(DP, None, None, CH),
        P(None, CH),
        P(None, CH),
        P(None, CH),
        P(None, CH),
        P(CH),
        P(CH, None),
        P(CH),
        P(),
    )
    out_specs = (
        P(DP, None, None, CH),
        P(DP, None, None, CH),
        P(None, CH),
        P(None, CH),
        P(None, CH),
        P(DP, CH),
        P(CH),
        P(CH, DP),
        P(CH),
    )
    return jax.shard_map(body, mesh=split, in_specs=in_specs, out_specs=out_specs, check_vma=False)
```

```python
import jax
import jax.numpy as jnp
from jax import lax
from jax.experimental import pallas as pl
from jax.experimental.pallas import tpu as pltpu
from jax.sharding import Mesh
from jax.sharding import PartitionSpec as P


KS = 7
DP = ("z", "y")
CH = ("x", "c")
SWAP = [(0, 1), (1, 0)]
EPS = 1e-05


def sent_to_all(array, axis):
    size = lax.axis_size(axis)
    return lax.all_to_all(
        jnp.broadcast_to(array[None], (size, *array.shape)), axis, 0, 0, tiled=True
    )


def rows_of_all(array):
    rows, own = array.shape
    halves = jnp.broadcast_to(array.reshape(1, 2, rows // 2, own), (4, 2, rows // 2, own))
    return lax.all_to_all(halves.reshape(8, rows // 2, own), CH, 0, 0, tiled=True)


def ring_scattered(array, axis):
    here = lax.axis_index(axis)

    def piece(k):
        return lax.dynamic_index_in_dim(array, (here + k) % 4, 0, keepdims=False)

    terms = [piece(0)] + [
        lax.ppermute(piece(k), axis, [(i, (i + k) % 4) for i in range(4)]) for k in (2, 1, 3)
    ]
    return sum(term.astype(jnp.float32) for term in terms)


REACH = KS // 2
TAPS = KS * KS


def spread(field, pad, planes):
    height, width, lanes = field.shape
    pad[:, :8] = jnp.zeros((height, 8, lanes), jnp.float32)
    pad[:, width + 8 :] = jnp.zeros((height, 8, lanes), jnp.float32)
    edge = jnp.zeros((KS, REACH, width, lanes), jnp.float32)
    planes[:, :REACH] = edge
    planes[:, height + REACH :] = edge

    @pl.loop(0, height)
    def _(r):
        pad[r, 8 : width + 8] = field[r].astype(jnp.float32)
        for b in range(KS):
            planes[b, r + REACH] = pad[r, 8 - REACH + b : 8 - REACH + b + width]


BLOCK = 4


def filtered_rows(planes, kernel, start, reverse=False):
    totals = [None] * BLOCK
    for b in range(KS):
        for t in range(BLOCK + KS - 1):
            window = planes[b, start + t]
            for i in range(BLOCK):
                if 0 <= t - i < KS:
                    tap = (t - i) * KS + b
                    tap = TAPS - 1 - tap if reverse else tap
                    term = window * kernel[tap : tap + 1]
                    totals[i] = term if totals[i] is None else totals[i] + term
    return totals


def folded(value):
    return jnp.sum(value.reshape(-1, 8, value.shape[-1]), axis=0)


def tap_sums(planes, upstream, height, width, store, plain=None):
    zero = jnp.zeros((8, planes.shape[-1]), jnp.float32)
    for b in range(KS):

        def step(block, sums):
            start = block * BLOCK
            sums = list(sums)
            for j in range(width // 8):
                cols = pl.ds(8 * j, 8)
                ups = [upstream(start + i, cols) for i in range(BLOCK)]
                for t in range(BLOCK + KS - 1):
                    window = planes[b, start + t, cols]
                    for i in range(BLOCK):
                        if 0 <= t - i < KS:
                            sums[t - i] = sums[t - i] + window * ups[i]
                            if plain is not None:
                                sums[KS + t - i] = sums[KS + t - i] + window
            return tuple(sums)

        count = KS if plain is None else 2 * KS
        sums = lax.fori_loop(0, height // BLOCK, step, (zero,) * count)
        for a in range(KS):
            store(a * KS + b, jnp.sum(sums[a], axis=0, keepdims=True))
            if plain is not None:
                plain(a * KS + b, jnp.sum(sums[KS + a], axis=0, keepdims=True))


def row_store(ref, first):
    def store(tap, row):
        ref[tap // 2, pl.ds(first + tap % 2, 1)] = row

    return store


def filter_kernel(*refs):
    filtered, moments, d_branch, pad, planes = refs[4:9]
    source, cotangent, scale, kernel = refs[9:13]
    copies = [
        pltpu.make_async_copy(refs[i], refs[9 + i], refs[13].at[i]) for i in range(4)
    ]
    for copy in copies:
        copy.start()
    for copy in copies:
        copy.wait()
    spread(source, pad, planes)
    zero = jnp.zeros((8, kernel.shape[1]), jnp.float32)

    def step(block, sums):
        start = block * BLOCK
        first, second = sums
        for i, row in enumerate(filtered_rows(planes, kernel, start)):
            r = start + i
            filtered[r] = row
            d_branch[r] = (cotangent[r].astype(jnp.float32) * scale[...]).astype(jnp.bfloat16)
            first, second = first + folded(row), second + folded(row * row)
        return first, second

    sums = lax.fori_loop(0, source.shape[0] // BLOCK, step, (zero, zero))
    for i in range(2):
        row = jnp.sum(sums[i], axis=0, keepdims=True)
        moments[:, i : i + 1] = jnp.broadcast_to(row[None], (moments.shape[0], *row.shape))


def terms_kernel(source, filtered, mean, sent, pad, planes):
    height, width, _ = source.shape
    sent[...] = jnp.zeros_like(sent)
    spread(source, pad, planes)
    tap_sums(
        planes,
        lambda r, cols: filtered[r, cols] - mean[...],
        height,
        width,
        row_store(sent, 4),
        row_store(sent, 2),
    )


def gather_kernel(
    pieces, source, filtered, rows, bias, base, d_normed, sent, pad, planes
):
    height, width, lanes = source.shape
    mean, rstd, scale, scaled = (rows[i : i + 1] for i in range(4))
    sent[...] = base[...]
    spread(source, pad, planes)
    zero = jnp.zeros((8, lanes), jnp.float32)

    def step(r, carry):
        side = r // (height // 2)
        here = pl.ds(pl.multiple_of((r - side * (height // 2)) * width, width), width)
        row = pieces[side, here].astype(jnp.float32)
        for x in range(1, 4):
            row = row + pieces[2 * x + side, here].astype(jnp.float32)
        d_normed[r] = row
        centered = (filtered[r] - mean) * rstd
        return carry[0] + folded(row * centered), carry[1] + folded(row)

    carry = lax.fori_loop(0, height, step, (zero, zero))
    for i in range(2):
        row = jnp.sum(carry[i], axis=0, keepdims=True)
        sent[:, 6 + i : 7 + i] = jnp.broadcast_to(row[None], (sent.shape[0], 1, lanes))
    tail = pieces[0, pl.ds(height * width // 2, 16)].astype(jnp.float32)
    for k in range(1, 8):
        tail = tail + pieces[k, pl.ds(height * width // 2, 16)].astype(jnp.float32)
    store = row_store(sent, 0)
    for q in range(4):
        store(TAPS + q, bias[:, q * lanes : (q + 1) * lanes])
    store(TAPS + 4, jnp.sum(tail, axis=0, keepdims=True) / scale)
    tap_sums(
        planes,
        lambda r, cols: d_normed[r, cols],
        height,
        width,
        lambda tap, row: store(tap, scaled * row),
    )


def input_kernel(d_normed, filtered, cotangent, kernel, rows, d_input, field, pad, planes):
    height = d_normed.shape[0]
    mean, rstd, scaled, shift, slope = (rows[i : i + 1] for i in range(5))

    @pl.loop(0, height)
    def _(r):
        centered = (filtered[r] - mean) * rstd
        field[r] = scaled * (d_normed[r] - shift - centered * slope)

    spread(field, pad, planes)

    @pl.loop(0, height // BLOCK)
    def _(block):
        start = block * BLOCK
        for i, row in enumerate(filtered_rows(planes, kernel, start, reverse=True)):
            r = start + i
            d_input[r] = (cotangent[r].astype(jnp.float32) + row).astype(jnp.bfloat16)


def conv_scratch(shape):
    height, width, lanes = shape
    return (
        pltpu.VMEM((height, width + 16, lanes), jnp.float32),
        pltpu.VMEM((KS, height + 2 * REACH, width, lanes), jnp.float32),
    )


GELU_A = 0.7978845608028654
GELU_B = 0.044715
TILE = 512
DOT_ROWS = (((0,), (0,)), ((), ()))
DOT_PLAIN = (((1,), (0,)), ((), ()))
DOT_COLS = (((1,), (1,)), ((), ()))


def dot(a, b, dims):
    return lax.dot_general(a, b, dims, preferred_element_type=jnp.float32)


def in_hbm(array):
    return pltpu.with_memory_space_constraint(array, pltpu.HBM)


def kernel_call(kernel, outs, operands, flops, scalar=False, scratch=(), space=pltpu.VMEM):
    vmem = pl.BlockSpec(memory_space=pltpu.VMEM)
    specs = [pl.BlockSpec(memory_space=space)] * len(operands)
    if scalar:
        specs[0] = pl.BlockSpec(memory_space=pltpu.SMEM)
    return pl.pallas_call(
        kernel,
        out_shape=[jax.ShapeDtypeStruct(s, t) for s, t in outs],
        in_specs=specs,
        out_specs=[vmem] * len(outs),
        scratch_shapes=list(scratch),
        cost_estimate=pl.CostEstimate(flops=flops, bytes_accessed=8 << 20, transcendentals=0),
        compiler_params=pltpu.CompilerParams(vmem_limit_bytes=24 << 20),
    )(*operands)


def joined(pieces, start, size):
    return jnp.concatenate([pieces[k, pl.ds(start, size)] for k in range(8)], axis=1)


def pointwise_kernel(core, z, y_all, w_own, w_pair, b_own, b_pair, v_own_far, v_pair_far, *rest):
    results, rest = rest[:4], rest[4:]
    bias_o, bias_p, held, slopes, scale, v_own, v_pair, pair, own, sems = rest
    act_o, act_p, back_o, back_p, out, grad_out = held[:6]
    y = held[7]
    half = z.shape[1]
    fetched = pltpu.make_async_copy(
        y_all.at[:, pl.ds(pl.multiple_of(core[0] * half, half), half)], y, sems.at[half // TILE, 1]
    )
    fetched = [
        fetched,
        pltpu.make_async_copy(v_own_far, v_own, sems.at[half // TILE, 2]),
        pltpu.make_async_copy(v_pair_far, v_pair, sems.at[half // TILE, 3]),
    ]
    for copy_in in fetched:
        copy_in.start()
    tiles = half // TILE
    bias_o[...] = jnp.zeros_like(bias_o)
    bias_p[...] = jnp.zeros_like(bias_p)
    scale[...] = jnp.zeros_like(scale)

    def copy(m, j):
        rows = pl.ds(pl.multiple_of(m * TILE, TILE), TILE)
        at = (slice(None), rows)
        return pltpu.make_async_copy(held[j].at[at], results[j - 4].at[at], sems.at[m, j])

    @pl.loop(0, tiles)
    def _(m):
        start = pl.multiple_of(m * TILE, TILE)
        rows = pl.ds(start, TILE)
        x = joined(z, start, TILE)
        for w, b, slope, act in (
            (w_own, b_own, slopes[0], act_o),
            (w_pair, b_pair, slopes[1], act_p),
        ):
            hidden = dot(x, w[...], DOT_PLAIN) + b[...]
            square = hidden * hidden
            t = jnp.tanh(GELU_A * (hidden + GELU_B * (square * hidden)))
            part = 0.5 * (1.0 + t)
            act[rows] = (hidden * part).astype(jnp.bfloat16)
            slope[...] = part + (0.5 * GELU_A) * hidden * (1.0 - t * t) * (
                1.0 + 3.0 * GELU_B * square
            )

        @pl.when(m == 0)
        def _():
            for copy_in in fetched:
                copy_in.wait()

        up = joined(y, start, TILE)
        for v, slope, back, bias in (
            (v_own, slopes[0], back_o, bias_o),
            (v_pair, slopes[1], back_p, bias_p),
        ):
            grad = dot(up, v[...], DOT_COLS) * slope[...]
            bias[...] += jnp.sum(grad, axis=0, keepdims=True)
            back[rows] = grad.astype(jnp.bfloat16)
        total = dot(back_o[rows], w_own[...], DOT_COLS) + dot(back_p[rows], w_pair[...], DOT_COLS)
        for k in range(8):
            grad_out[k, rows] = total[:, k * 128 : (k + 1) * 128].astype(jnp.bfloat16)
        copy(m, 5).start()
        total = dot(act_o[rows], v_own[...], DOT_PLAIN) + dot(act_p[rows], v_pair[...], DOT_PLAIN)
        for k in range(8):
            out[k, rows] = total[:, k * 128 : (k + 1) * 128].astype(jnp.bfloat16)
        copy(m, 4).start()
        scale[...] += jnp.sum(up.astype(jnp.float32) * total, axis=0, keepdims=True)

    for k in range(8):
        value = scale[:, k * 128 : (k + 1) * 128]
        high = value.astype(jnp.bfloat16).astype(jnp.float32)
        row = lax.broadcasted_iota(jnp.int32, (16, 128), 0)
        both = jnp.where(row == 0, high, jnp.where(row == 1, value - high, 0.0))
        held[6][k] = both.astype(jnp.bfloat16)
    last = pltpu.make_async_copy(
        held[6], results[1].at[:, pl.ds(half, 16)], sems.at[tiles, 0]
    )
    last.start()

    def grad_copy(k, i):
        here = pl.ds(pl.multiple_of(k * 256, 256), 256)
        grads = (pair, own)[i]
        return pltpu.make_async_copy(
            grads.at[here], results[2 + i].at[here], sems.at[tiles + 1 + i, k]
        )

    width = back_p.shape[1]
    for i, (grads, back, act) in enumerate(((pair, back_p, act_p), (own, back_o, act_o))):

        @pl.loop(0, 4)
        def _(k):
            here = pl.ds(pl.multiple_of(k * 256, 256), 256)
            x = jnp.concatenate([z[2 * k], z[2 * k + 1]], axis=1)
            up = jnp.concatenate([y[2 * k], y[2 * k + 1]], axis=1)
            grads[here, :width] = dot(x, back[...], DOT_ROWS).astype(jnp.bfloat16)
            grads[here, width:] = dot(up, act[...], DOT_ROWS).astype(jnp.bfloat16)
            grad_copy(k, i).start()

    for m in range(tiles):
        for j in (4, 5):
            copy(m, j).wait()
    last.wait()
    for i in range(2):
        for k in range(4):
            grad_copy(k, i).wait()


def pointwise_pass(core, z, y, w_own, w_pair, b_own, b_pair, v_own, v_pair):
    rows, width = z.shape[1], w_own.shape[1]
    vmem = pl.BlockSpec(memory_space=pltpu.VMEM)
    flat, wide = (rows, width), (8, rows, 128)
    outs = [wide, (8, rows + 16, 128)] + [(1024, 2 * width)] * 2
    held = tuple(pltpu.VMEM(s, jnp.bfloat16) for s in [flat] * 4 + [wide, wide, (8, 16, 128), wide])
    return pl.pallas_call(
        lambda *refs: pointwise_kernel(*refs[:15], refs[15:23], refs[23:25], *refs[25:]),
        out_shape=[pltpu.HBM(s, jnp.bfloat16) for s in outs]
        + [jax.ShapeDtypeStruct((1, width), jnp.float32)] * 2,
        in_specs=[pl.BlockSpec(memory_space=pltpu.SMEM), vmem]
        + [pl.BlockSpec(memory_space=pltpu.HBM)]
        + [vmem] * 4
        + [pl.BlockSpec(memory_space=pltpu.HBM)] * 2,
        out_specs=[pl.BlockSpec(memory_space=pltpu.HBM)] * 4 + [vmem] * 2,
        scratch_shapes=[
            *held,
            pltpu.VMEM((TILE, width), jnp.float32),
            pltpu.VMEM((TILE, width), jnp.float32),
            pltpu.VMEM((1, 1024), jnp.float32),
            pltpu.VMEM(v_own.shape, jnp.bfloat16),
            pltpu.VMEM(v_own.shape, jnp.bfloat16),
            pltpu.VMEM((1024, 2 * width), jnp.bfloat16),
            pltpu.VMEM((1024, 2 * width), jnp.bfloat16),
            pltpu.SemaphoreType.DMA((rows // TILE + 3, 6)),
        ],
        cost_estimate=pl.CostEstimate(
            flops=16 * rows * width * 1024, bytes_accessed=8 << 20, transcendentals=0
        ),
        compiler_params=pltpu.CompilerParams(vmem_limit_bytes=36 << 20),
    )(
        core,
        z,
        in_hbm(y),
        w_own,
        w_pair,
        b_own[None],
        b_pair[None],
        in_hbm(v_own),
        in_hbm(v_pair),
    )


def body(
    activations,
    cotangent,
    dw_kernel,
    norm_gain,
    norm_bias,
    w_in,
    b_in,
    w_out,
    layer_scale,
    group_sizes,
):
    channels = activations.shape[3]
    row_count = activations.shape[1] * activations.shape[2]
    core = lax.axis_index("c")
    devices = lax.axis_size(DP)
    position = lax.axis_index(DP)
    groups = group_sizes.shape[0]
    group_ends = jnp.cumsum(group_sizes)
    positions = jnp.arange(devices, dtype=jnp.int32)
    labels = jnp.sum((group_ends[None, :] <= positions[:, None]).astype(jnp.int32), axis=1)
    own_group = jnp.sum((group_ends <= position).astype(jnp.int32))
    owners = (jnp.arange(groups, dtype=jnp.int32)[:, None] == labels[None, :]).astype(jnp.float32)
    member = (jnp.arange(groups, dtype=jnp.int32) == own_group).astype(jnp.float32)
    own_count = jnp.sum(member * group_sizes.astype(jnp.float32)) * row_count
    own_gain = jnp.sum(member[:, None] * norm_gain, axis=0)
    own_bias = jnp.sum(member[:, None] * norm_bias, axis=0)

    w_in_pair = lax.ppermute(w_in, "c", SWAP)
    w_out_pair = lax.ppermute(w_out, "c", SWAP)
    b_in_pair = lax.ppermute(b_in, "c", SWAP)

    image = activations.shape[1:]
    source = activations[0]
    scratch = conv_scratch(image)
    operands = (source, cotangent[0], layer_scale[None], dw_kernel)
    filtered, moments, d_branch = kernel_call(
        filter_kernel,
        [(image, jnp.float32), ((devices, 2, channels), jnp.float32), (image, jnp.bfloat16)],
        tuple(in_hbm(a) for a in operands),
        1 << 29,
        scratch=(
            *scratch,
            *(pltpu.VMEM(a.shape, a.dtype) for a in operands),
            pltpu.SemaphoreType.DMA((4,)),
        ),
        space=pltpu.HBM,
    )
    everyone = lax.all_gather(d_branch.reshape(row_count, channels), CH)
    per_device = lax.all_to_all(moments, DP, 0, 0, tiled=True)
    counts = group_sizes.astype(jnp.float32)[:, None] * row_count
    totals = jnp.sum(owners[:, :, None, None] * per_device[None], axis=1)
    group_mean = totals[:, 0] / counts
    group_rstd = lax.rsqrt(totals[:, 1] / counts - group_mean * group_mean + EPS)
    own_mean = jnp.sum(member[:, None] * group_mean, axis=0)
    own_rstd = jnp.sum(member[:, None] * group_rstd, axis=0)
    centered = (filtered.reshape(row_count, channels) - own_mean) * own_rstd
    normed = (centered * own_gain + own_bias).astype(jnp.bfloat16)
    (base,) = kernel_call(
        terms_kernel,
        [((devices, 8, channels), jnp.float32)],
        (source, filtered, moments[0, :1] / row_count),
        1 << 29,
        scratch=scratch,
    )
    gathered = rows_of_all(normed)
    gathered, base = lax.optimization_barrier((gathered, base))

    where = core.astype(jnp.int32)[None]
    (
        partial_branch,
        partial_normed,
        for_pair,
        own_grads,
        bias_own,
        bias_pair,
    ) = pointwise_pass(where, gathered, everyone, w_in, w_in_pair, b_in, b_in_pair, w_out, w_out_pair)
    normed_pieces = lax.all_to_all(partial_normed, CH, 0, 0, tiled=True)
    from_pair = lax.ppermute(for_pair, "c", SWAP)
    both_local = own_grads.astype(jnp.float32) + from_pair.astype(jnp.float32)
    both_local = both_local.astype(jnp.bfloat16)
    hidden_cols = w_in.shape[1]
    bias_local = bias_own + lax.ppermute(bias_pair, "c", SWAP)
    near = lax.psum_scatter(both_local, "z", scatter_dimension=0, tiled=True)

    from_mean = per_device[:, 0] / row_count - jnp.sum(
        owners[:, :, None] * group_mean[:, None], axis=0
    )
    own_scaled = own_gain * own_rstd
    d_normed, sent = kernel_call(
        gather_kernel,
        [(image, jnp.float32), (base.shape, jnp.float32)],
        (
            normed_pieces,
            source,
            filtered,
            jnp.stack([own_mean, own_rstd, layer_scale, own_scaled]),
            bias_local,
            base,
        ),
        1 << 29,
        scratch=scratch,
    )
    sent, partial_branch = lax.optimization_barrier((sent, partial_branch))
    parts = lax.all_to_all(sent, DP, 0, 0, tiled=True)
    halves = (4, 2, row_count // 2, channels)
    chip_branch = ring_scattered(partial_branch.reshape(halves), "x").astype(jnp.bfloat16)
    kept = lax.dynamic_index_in_dim(chip_branch, core, 0, keepdims=False)
    given = lax.dynamic_index_in_dim(chip_branch, 1 - core, 0, keepdims=False)
    taken = lax.ppermute(given, "c", SWAP)
    branch = jnp.concatenate(
        [jnp.where(core == 0, kept, taken), jnp.where(core == 0, taken, kept)]
    ).astype(jnp.float32)
    initial = activations.reshape(row_count, channels).astype(jnp.float32)
    result = (initial + layer_scale * branch).astype(jnp.bfloat16)
    result = result.reshape(activations.shape)
    grad_totals = jnp.sum(owners[:, :, None, None] * parts[None, :, 6:], axis=1)
    d_gain = grad_totals[:, 0]
    d_bias = grad_totals[:, 1]
    from_mean = per_device[:, 0] / row_count - jnp.sum(
        owners[:, :, None] * group_mean[:, None], axis=0
    )
    rest_parts = parts[:, 4:6] + from_mean[:, None] * parts[:, 2:4]
    scaled_all = norm_gain * group_rstd / counts
    flat_weight = jnp.sum(owners[:, :, None] * (scaled_all * d_bias)[:, None], axis=0)
    rest_weight = jnp.sum(
        owners[:, :, None] * (scaled_all * group_rstd * d_gain)[:, None], axis=0
    )
    piece = jnp.sum(
        parts[:, :2]
        - flat_weight[:, None] * parts[:, 2:4]
        - rest_weight[:, None] * rest_parts,
        axis=0,
    )
    total = sent_to_all(piece, DP).reshape(64, channels)
    d_kernel = total[:TAPS]
    d_b_in = total[TAPS : TAPS + 4].ravel()
    d_scale = total[TAPS + 4]
    own_dgain = jnp.sum(member[:, None] * d_gain, axis=0)
    own_dbias = jnp.sum(member[:, None] * d_bias, axis=0)
    rows = jnp.stack(
        [own_mean, own_rstd, own_scaled, own_dbias / own_count, own_dgain / own_count]
    )
    (d_input,) = kernel_call(
        input_kernel,
        [(image, jnp.bfloat16)],
        (d_normed, filtered, cotangent[0], dw_kernel, rows),
        1 << 29,
        scratch=(pltpu.VMEM(image, jnp.float32), *scratch),
    )
    d_input = d_input[None]
    both_sums = ring_scattered(near.reshape(4, -1, near.shape[1]), "y")
    d_w_in = both_sums[:, :hidden_cols]
    d_w_out = both_sums[:, hidden_cols:].T
    return (result, d_input, d_kernel, d_gain, d_bias, d_w_in, d_b_in, d_w_out, d_scale)


def solution(mesh):
    split = Mesh(mesh.devices.reshape(8, 4, 4, 2), ("z", "y", "x", "c"))
    in_specs = (
        P(DP, None, None, CH),
        P(DP, None, None, CH),
        P(None, CH),
        P(None, CH),
        P(None, CH),
        P(None, CH),
        P(CH),
        P(CH, None),
        P(CH),
        P(),
    )
    out_specs = (
        P(DP, None, None, CH),
        P(DP, None, None, CH),
        P(None, CH),
        P(None, CH),
        P(None, CH),
        P(DP, CH),
        P(CH),
        P(CH, DP),
        P(CH),
    )
    return jax.shard_map(body, mesh=split, in_specs=in_specs, out_specs=out_specs, check_vma=False)
```
